512 devices in a mesh: gx: 4 (over y_hi, core), gy: 16 (over z), gz: 8 (over y_lo, x).
Axes of the slice: x: 4, y: 4 (y_hi: 2, y_lo: 2; y = y_hi * 2 + y_lo), z: 16, core: 2. Of those that a mesh axis runs over, the one named last changes fastest.
Arguments:
- heat_level_grid: float32 [256, 1024, 512], P('gz', 'gy', 'gx'), may hold values from -16 to 16, as said below
- interval_first_class: int32 [1], replicated, may hold values from 0 to 95
- interval_beyond_class: int32 [1], replicated, may hold values from 128 to 256
Outputs:
- magnitude: float32 [256, 1024, 512], P('gz', 'gy', 'gx')
- histogram: float32 [256], replicated
- stats: float32 [4], replicated
The draws below stay inside these ranges and needn't reach their ends.
Inputs may be any that keep to these rules, and one draw needn't show every extreme that they name: `heat_level_grid`: each entry is a rough value times an amplitude that is constant on blocks of 8 x 4 x 4 cells (z, y, x) and varies over a factor of 16 between blocks.
All inputs are finite; a program needn't handle non-finite values.
Results may differ from the reference program's by a relative error of at most 0.0003.
Values sent between devices are 32-bit elements; how exact they have to be, the bound alone decides.
A program may use at most 64 MiB of HBM per device.

```python
import math
import jax
import jax.numpy as jnp

BINS = 256
NX = 512
NY = 1024
NZ = 256


def draw_heat_level_grid(key, part):
    first_key, second_key = jax.random.split(jax.random.fold_in(key, 11))
    coarse = jax.random.uniform(first_key, (NZ // 8, NY // 4, NX // 4), jnp.float32, math.log(0.25), math.log(4.0))
    amplitude = jnp.exp(coarse)
    amplitude = jnp.repeat(jnp.repeat(jnp.repeat(amplitude, 8, axis=0), 4, axis=1), 4, axis=2)
    noise = jnp.clip(jax.random.normal(second_key, (NZ, NY, NX), jnp.float32), -4.0, 4.0)
    return (amplitude * noise).astype(jnp.float32)


def setup_inputs(seed: int = 0) -> dict:
    key_list = jax.random.split(jax.random.key(seed), 4)
    return {
        "heat_level_grid": draw_heat_level_grid(jax.random.fold_in(key_list[3], 71), 0),
        "interval_first_class": jax.random.randint(key_list[1], (1,), 0, 96).astype(jnp.int32),
        "interval_beyond_class": jax.random.randint(key_list[2], (1,), 128, BINS + 1).astype(jnp.int32),
    }


stencil_coefficients = (0.8, -0.2, 4.0 / 105.0, -1.0 / 280.0)
grad_range = 12.0

def directional_rate(field, direction_length_count):
    running = jnp.zeros_like(field)
    for offset, coefficient in enumerate(stencil_coefficients, start=1):
        running = running + coefficient * (jnp.roll(field, -offset, direction_length_count) - jnp.roll(field, offset, direction_length_count))
    return running

def reference(heat_level_grid, interval_first_class, interval_beyond_class):
    slope_norm_square = jnp.zeros_like(heat_level_grid)
    for direction_length_count in range(3):
        slope_in_direction = directional_rate(heat_level_grid, direction_length_count)
        slope_norm_square = slope_norm_square + slope_in_direction * slope_in_direction
    magnitude = jnp.sqrt(slope_norm_square + 1.0) - 1.0
    position = jnp.clip(magnitude * (BINS / grad_range), 0.5, BINS - 0.5)
    low_bin = jnp.minimum(jnp.floor(position - 0.5), BINS - 2).astype(jnp.int32)
    fraction = position - 0.5 - low_bin.astype(position.dtype)
    flat_low = low_bin.ravel()
    flat_frac = fraction.ravel()
    counts = jax.ops.segment_sum(1.0 - flat_frac, flat_low, BINS) + jax.ops.segment_sum(flat_frac, flat_low + 1, BINS)
    total_cells = NX * NY * NZ
    histogram = counts * (BINS / total_cells)
    lower_edge = interval_first_class[0]
    upper_edge = interval_beyond_class[0]
    high_bin = low_bin + 1
    inside_low = (low_bin >= lower_edge) & (low_bin < upper_edge)
    inside_high = (high_bin >= lower_edge) & (high_bin < upper_edge)
    weight = jnp.where(inside_low, 1.0 - fraction, 0.0) + jnp.where(inside_high, fraction, 0.0)
    lowest = jnp.min(magnitude + grad_range * (1.0 - weight))
    highest = jnp.max(weight * magnitude)
    weighted_sum = jnp.sum(weight * magnitude) / total_cells
    weighted_count = jnp.sum(weight) / total_cells
    stats = jnp.stack([lowest, highest, weighted_sum, weighted_count])
    return (magnitude, histogram, stats)
```

```python
import functools

import jax
import jax.numpy as jnp
from jax import lax
from jax.experimental import pallas as pl
from jax.experimental.pallas import tpu as pltpu
from jax.sharding import PartitionSpec as P

MESH = pl.DeviceIdType.MESH
BINS = 256
RANGE = 12.0
COEF = (0.8, -0.2, 4.0 / 105.0, -1.0 / 280.0)


def kernel(
    sizes, cells, edges, u_hbm, mag_ref, hist_ref, stat_ref,
    ext, packed, from_low, from_high, acc, msg, plane, line,
    in_sem, send_sem, recv_sem, plane_send, plane_recv, line_send, line_recv,
):
    nx, ny, nz = sizes
    dz, dy, dx = u_hbm.shape
    tiles = dy // 8
    gx, gy, gz = lax.axis_index("gx"), lax.axis_index("gy"), lax.axis_index("gz")

    def device(a=0, c=0, b=0):
        return {
            "gx": lax.rem(gx + (a + nx), nx),
            "gy": lax.rem(gy + (c + ny), ny),
            "gz": lax.rem(gz + (b + nz), nz),
        }

    plane_peers = [(a, b) for a in range(nx) for b in range(nz)][1:]

    own = ext.at[pl.ds(4, dz), pl.ds(8, dy), :]
    load = pltpu.make_async_copy(u_hbm, own, in_sem)
    load.start()
    barrier = pltpu.get_barrier_semaphore()
    for a, b in plane_peers:
        pl.semaphore_signal(barrier, inc=1, device_id=device(a=a, b=b), device_id_type=MESH)
    for c in range(1, ny):
        pl.semaphore_signal(barrier, inc=1, device_id=device(c=c), device_id_type=MESH)
    load.wait()

    lane = lax.broadcasted_iota(jnp.int32, (8, dx), 1)

    def pack(p, _):
        out = jnp.zeros((8, dx), jnp.float32)
        for j in range(16):
            cell = ext[4 + 2 * p + j // 8, pl.ds(8 + 8 * (j % 8), 8), :]
            moved = pltpu.roll(cell, 8 * j + 4, 1)
            out = jnp.where(lane // 8 == j, moved, out)
        packed[p] = out
        return 0

    lax.fori_loop(0, dz // 2, pack, 0)

    pl.semaphore_wait(barrier, len(plane_peers) + ny - 1)

    def send(k, src, dst, **offset):
        copy = pltpu.make_async_remote_copy(
            src_ref=src, dst_ref=dst, send_sem=send_sem.at[k], recv_sem=recv_sem.at[k],
            device_id=device(**offset), device_id_type=MESH,
        )
        copy.start()
        return copy

    rows = pl.ds(8, dy)
    planes = pl.ds(4, dz)
    copies = [
        send(0, ext.at[planes, pl.ds(8, 4), :], ext.at[planes, pl.ds(8 + dy, 4), :], c=-1),
        send(1, ext.at[planes, pl.ds(4 + dy, 4), :], ext.at[planes, pl.ds(4, 4), :], c=1),
        send(2, packed, from_high, a=-1),
        send(3, packed, from_low, a=1),
        send(4, ext.at[pl.ds(4, 4), rows, :], ext.at[pl.ds(4 + dz, 4), rows, :], b=-1),
        send(5, ext.at[pl.ds(dz, 4), rows, :], ext.at[pl.ds(0, 4), rows, :], b=1),
    ]
    acc[...] = jnp.zeros_like(acc)
    for copy in copies:
        copy.wait_send()
        copy.wait_recv()

    low_edge = edges[0].astype(jnp.float32) - 1.0
    high_edge = edges[1].astype(jnp.float32) - 1.0
    half = lax.broadcasted_iota(jnp.int32, (16, dx), 0) // 8
    half = half.astype(jnp.float32)

    def pair(x):
        return jnp.concatenate([x, x], axis=0)

    def one_slab(p, carry):
        wsum, wmax, wmin = carry
        rims = jnp.where(lane % 8 < 4, from_low[p], from_high[p])
        lefts, rights = [], []
        for j in range(16):
            z, y = 4 + 2 * p + j // 8, 8 + 8 * (j % 8)
            center = ext[z, pl.ds(y, 8), :]
            rim = pltpu.roll(rims, (dx - 8 * j - 4) % dx, 1)
            grad_x = grad_y = grad_z = None
            for k, coef in enumerate(COEF, start=1):
                ahead = pltpu.roll(jnp.where(lane < k, rim, center), dx - k, 1)
                behind = pltpu.roll(jnp.where(lane >= dx - k, rim, center), k, 1)
                term_x = coef * (ahead - behind)
                term_y = coef * (ext[z, pl.ds(y + k, 8), :] - ext[z, pl.ds(y - k, 8), :])
                term_z = coef * (ext[z + k, pl.ds(y, 8), :] - ext[z - k, pl.ds(y, 8), :])
                grad_x = term_x if grad_x is None else grad_x + term_x
                grad_y = term_y if grad_y is None else grad_y + term_y
                grad_z = term_z if grad_z is None else grad_z + term_z
            square = grad_z * grad_z + grad_y * grad_y + grad_x * grad_x
            magnitude = jnp.sqrt(square + 1.0) - 1.0
            mag_ref[2 * p + j // 8, pl.ds(8 * (j % 8), 8), :] = magnitude
            place = jnp.clip(magnitude * (BINS / RANGE) - 0.5, 0.0, BINS - 1.0)
            low = jnp.minimum(jnp.floor(place), BINS - 2.0)
            fraction = place - low
            weight = jnp.clip(place - low_edge, 0.0, 1.0) - jnp.clip(place - high_edge, 0.0, 1.0)
            value = weight * magnitude
            wsum = wsum + value
            wmax = jnp.maximum(wmax, value)
            wmin = jnp.minimum(wmin, (magnitude + RANGE) - RANGE * weight)
            coarse = jnp.floor(low * 0.125)
            fine = low - 8.0 * coarse
            coarse = (pair(coarse) - half).astype(jnp.bfloat16)
            fine = (pair(fine) - half).astype(jnp.bfloat16)
            part = fraction.astype(jnp.bfloat16)
            rest = (fraction - part.astype(jnp.float32)).astype(jnp.bfloat16)
            part, rest = pair(part), pair(rest)
            one = jnp.ones((16, dx), jnp.bfloat16)
            zero = jnp.zeros((16, dx), jnp.bfloat16)
            lefts.append(
                jnp.concatenate(
                    [jnp.where(coarse == jnp.bfloat16(2 * k), one, zero) for k in range(16)], axis=0
                )
            )
            hits = [fine == jnp.bfloat16(2 * k) for k in range(4)]
            rights.append(
                jnp.concatenate(
                    [jnp.where(hit, term, zero) for term in (one, part, rest) for hit in hits], axis=0
                )
            )
        acc[...] += lax.dot_general(
            jnp.concatenate(lefts, axis=1), jnp.concatenate(rights, axis=1),
            (((1,), (1,)), ((), ())), preferred_element_type=jnp.float32,
        )
        return wsum, wmax, wmin

    nothing = jnp.zeros((8, dx), jnp.float32)
    wsum, wmax, wmin = lax.fori_loop(
        0, dz // 2, one_slab, (nothing, nothing, jnp.full((8, dx), 1e30, jnp.float32))
    )

    total = acc[...]
    same = (
        lax.broadcasted_iota(jnp.int32, total.shape, 0) % 8
        == lax.broadcasted_iota(jnp.int32, total.shape, 1) % 8
    )
    total = jnp.where(same, total, 0.0).reshape(32, 8, 192).sum(axis=1)
    source = lax.broadcasted_iota(jnp.int32, (192, 128), 0)
    target = lax.broadcasted_iota(jnp.int32, (192, 128), 1)
    fits = (source // 8) % 8 == target % 8
    coarse_row = lax.broadcasted_iota(jnp.int32, (32, 128), 0)
    coarse_lane = lax.broadcasted_iota(jnp.int32, (32, 128), 1)
    keep = coarse_row % 16 == coarse_lane // 8

    def bins_of(chosen):
        spread = lax.dot_general(
            total, jnp.where(fits & chosen, 1.0, 0.0), (((1,), (0,)), ((), ())),
            precision=lax.Precision.HIGHEST, preferred_element_type=jnp.float32,
        )
        spread = jnp.where(keep, spread, 0.0)
        return spread[:16].sum(axis=0, keepdims=True), spread[16:].sum(axis=0, keepdims=True)

    number = bins_of(source < 64)
    part = bins_of(source >= 64)
    lane1 = lane[:1]
    turned = [pltpu.roll(pair(pair(pair(x))), 1, 1)[:1] for x in part]
    first = number[0] - part[0] + jnp.where(lane1 == 0, turned[1], turned[0])
    second = number[1] - part[1] + jnp.where(lane1 == 0, turned[0], turned[1])
    third = jnp.where(
        lane1 == 0, jnp.sum(wsum),
        jnp.where(lane1 == 1, jnp.max(wmax), jnp.min(wmin)),
    )
    msg[0:3, :] = jnp.concatenate([first, second, third], axis=0)

    def merged(slots, slot_ref):
        value = slot_ref[0]
        added, most, least = value, value, value
        for k in range(1, slots):
            value = slot_ref[k]
            added, most, least = added + value, jnp.maximum(most, value), jnp.minimum(least, value)
        lane3 = lax.broadcasted_iota(jnp.int32, added.shape, 1)
        row3 = lax.broadcasted_iota(jnp.int32, added.shape, 0)
        return jnp.where(
            (row3 < 2) | (lane3 == 0), added, jnp.where(lane3 == 1, most, least)
        )

    def exchange(peers, slot_ref, send_one, recv_one):
        slots = len(peers) + 1
        slot_ref[0] = msg[...]
        for k, offset in enumerate(peers, start=1):
            pltpu.make_async_remote_copy(
                src_ref=msg, dst_ref=slot_ref.at[k], send_sem=send_one, recv_sem=recv_one,
                device_id=device(**offset), device_id_type=MESH,
            ).start()
        rest = slot_ref.at[pl.ds(1, slots - 1)]
        pltpu.make_async_copy(rest, rest, send_one).wait()
        pltpu.make_async_copy(rest, rest, recv_one).wait()
        return merged(slots, slot_ref)

    msg[...] = exchange([dict(a=a, b=b) for a, b in plane_peers], plane, plane_send, plane_recv)
    done = exchange([dict(c=c) for c in range(1, ny)], line, line_send, line_recv)

    hist_ref[...] = done[0:2] * (BINS / cells)
    bin_id = lax.broadcasted_iota(jnp.int32, (2, 128), 0) * 128 + lax.broadcasted_iota(
        jnp.int32, (2, 128), 1
    )
    inside = (bin_id >= edges[0]) & (bin_id < edges[1])
    number = jnp.sum(jnp.where(inside, done[0:2], 0.0))
    last = done[2:3]
    total, most, least = (
        jnp.sum(jnp.where(lane1 == k, last, 0.0)) for k in range(3)
    )
    stat_ref[...] = jnp.where(
        lane1 == 0, least,
        jnp.where(lane1 == 1, most, jnp.where(lane1 == 2, total, number) * (1.0 / cells)),
    )


def solution(mesh):
    sizes = tuple(mesh.shape[name] for name in ("gx", "gy", "gz"))
    nx, ny, nz = sizes

    def on_device(u, first, beyond):
        dz, dy, dx = u.shape
        cells = u.size * nx * ny * nz
        edges = jnp.concatenate([first, beyond])
        magnitude, hist, stat = pl.pallas_call(
            functools.partial(kernel, sizes, cells),
            out_shape=(
                jax.ShapeDtypeStruct(u.shape, jnp.float32),
                jax.ShapeDtypeStruct((2, 128), jnp.float32),
                jax.ShapeDtypeStruct((1, 128), jnp.float32),
            ),
            in_specs=[
                pl.BlockSpec(memory_space=pltpu.SMEM),
                pl.BlockSpec(memory_space=pl.ANY),
            ],
            out_specs=(
                pl.BlockSpec(memory_space=pltpu.VMEM),
                pl.BlockSpec(memory_space=pltpu.VMEM),
                pl.BlockSpec(memory_space=pltpu.VMEM),
            ),
            scratch_shapes=[
                pltpu.VMEM((dz + 8, dy + 16, dx), jnp.float32),
                pltpu.VMEM((dz // 2, 8, dx), jnp.float32),
                pltpu.VMEM((dz // 2, 8, dx), jnp.float32),
                pltpu.VMEM((dz // 2, 8, dx), jnp.float32),
                pltpu.VMEM((256, 192), jnp.float32),
                pltpu.VMEM((3, 128), jnp.float32),
                pltpu.VMEM((nx * nz, 3, 128), jnp.float32),
                pltpu.VMEM((ny, 3, 128), jnp.float32),
                pltpu.SemaphoreType.DMA,
                pltpu.SemaphoreType.DMA((6,)),
                pltpu.SemaphoreType.DMA((6,)),
                pltpu.SemaphoreType.DMA,
                pltpu.SemaphoreType.DMA,
                pltpu.SemaphoreType.DMA,
                pltpu.SemaphoreType.DMA,
            ],
            compiler_params=pltpu.CompilerParams(collective_id=0, has_side_effects=True),
        )(edges, u)
        return magnitude, hist.reshape(BINS), stat[0, :4]

    return jax.shard_map(
        on_device,
        mesh=mesh,
        in_specs=(P("gz", "gy", "gx"), P(), P()),
        out_specs=(P("gz", "gy", "gx"), P(), P()),
        check_vma=False,
    )
```

```python
import functools

import jax
import jax.numpy as jnp
from jax import lax
from jax.experimental import pallas as pl
from jax.experimental.pallas import tpu as pltpu
from jax.sharding import PartitionSpec as P

MESH = pl.DeviceIdType.MESH
BINS = 256
RANGE = 12.0
COEF = (0.8, -0.2, 4.0 / 105.0, -1.0 / 280.0)


def pair(x):
    return jnp.concatenate([x, x], axis=0)


def kernel(
    sizes, cells, u_hbm, first_hbm, beyond_hbm, mag_ref, hist_ref, stat_ref,
    ext, packed, from_low, from_high, rim_x, rim_yz, acc, msg, plane, line, first, beyond,
    in_sem, edge_sem, send_sem, recv_sem, plane_send, plane_recv, line_send, line_recv,
    near2, near3, far2, far3,
):
    nx, ny, nz = sizes
    dz, dy, dx = u_hbm.shape
    gx, gy, gz = lax.axis_index("gx"), lax.axis_index("gy"), lax.axis_index("gz")

    def device(a=0, c=0, b=0):
        return {
            "gx": lax.rem(gx + (a + nx), nx) if a else gx,
            "gy": lax.rem(gy + (c + ny), ny) if c else gy,
            "gz": lax.rem(gz + (b + nz), nz) if b else gz,
        }

    def signal(sem, **offset):
        pl.semaphore_signal(sem, inc=1, device_id=device(**offset), device_id_type=MESH)

    load = pltpu.make_async_copy(u_hbm, ext.at[pl.ds(4, dz), pl.ds(8, dy), :], in_sem)
    load.start()
    barrier = pltpu.get_barrier_semaphore()
    for offset in (dict(a=-1), dict(a=1), dict(c=-1), dict(c=1), dict(b=-1), dict(b=1)):
        signal(barrier, **offset)
    edge_loads = [
        pltpu.make_async_copy(first_hbm, first, edge_sem.at[0]),
        pltpu.make_async_copy(beyond_hbm, beyond, edge_sem.at[1]),
    ]
    for copy in edge_loads:
        copy.start()

    lane = lax.broadcasted_iota(jnp.int32, (8, dx), 1)
    slot = lane // 8
    left_rim = lane % 8 < 4
    lane16 = lax.broadcasted_iota(jnp.int32, (16, dx), 1)
    half = (lax.broadcasted_iota(jnp.int32, (16, dx), 0) // 8).astype(jnp.float32)
    half_core = jnp.where((lane16 < 4) | (lane16 >= dx - 4), 1000.0, half)
    rim_lane = (lane < 4) | (lane >= dx - 4)

    load.wait()

    def pack(i, _):
        for p in (4 * i, 4 * i + 1, 4 * i + 2, 4 * i + 3):
            out = jnp.zeros((8, dx), jnp.float32)
            for j in range(16):
                cell = ext[4 + 2 * p + j // 8, pl.ds(8 + 8 * (j % 8), 8), :]
                out = jnp.where(slot == j, pltpu.roll(cell, 8 * j + 4, 1), out)
            packed[p] = out
        return 0

    lax.fori_loop(0, dz // 8, pack, 0)

    pl.semaphore_wait(barrier, 6)

    def send(k, src, dst, **offset):
        copy = pltpu.make_async_remote_copy(
            src_ref=src, dst_ref=dst, send_sem=send_sem.at[k], recv_sem=recv_sem.at[k],
            device_id=device(**offset), device_id_type=MESH,
        )
        copy.start()
        return copy

    rows = pl.ds(8, dy)
    planes = pl.ds(4, dz)
    y_rims = [
        send(0, ext.at[planes, pl.ds(8, 4), :], ext.at[planes, pl.ds(8 + dy, 4), :], c=-1),
        send(1, ext.at[planes, pl.ds(4 + dy, 4), :], ext.at[planes, pl.ds(4, 4), :], c=1),
    ]
    xz_rims = [
        send(4, ext.at[pl.ds(4, 4), rows, :], ext.at[pl.ds(4 + dz, 4), rows, :], b=-1),
        send(5, ext.at[pl.ds(dz, 4), rows, :], ext.at[pl.ds(0, 4), rows, :], b=1),
        send(2, packed, from_high, a=-1),
        send(3, packed, from_low, a=1),
    ]
    acc[...] = jnp.zeros_like(acc)
    for copy in edge_loads:
        copy.wait()
    low_edge = first[0].astype(jnp.float32) - 1.0
    high_edge = beyond[0].astype(jnp.float32) - 1.0

    def classify(square, halves, stats):
        wsum, wmax, wmin = stats
        magnitude = jnp.sqrt(square + 1.0) - 1.0
        place = jnp.clip(magnitude * (BINS / RANGE) - 0.5, 0.0, BINS - 1.0)
        low = jnp.minimum(jnp.floor(place), BINS - 2.0)
        fraction = place - low
        weight = jnp.clip(place - low_edge, 0.0, 1.0) - jnp.clip(place - high_edge, 0.0, 1.0)
        value = weight * magnitude
        stats = (
            wsum + value,
            jnp.maximum(wmax, value),
            jnp.minimum(wmin, (magnitude + RANGE) - RANGE * weight),
        )
        coarse = jnp.floor(low * 0.125)
        fine = low - 8.0 * coarse
        coarse = (pair(coarse) - halves).astype(jnp.bfloat16)
        fine = (pair(fine) - half).astype(jnp.bfloat16)
        part = fraction.astype(jnp.bfloat16)
        rest = (fraction - part.astype(jnp.float32)).astype(jnp.bfloat16)
        part, rest = pair(part), pair(rest)
        one = jnp.ones((16, dx), jnp.bfloat16)
        zero = jnp.zeros((16, dx), jnp.bfloat16)
        left = jnp.concatenate(
            [jnp.where(coarse == jnp.bfloat16(2 * k), one, zero) for k in range(16)], axis=0
        )
        hits = [fine == jnp.bfloat16(2 * k) for k in range(4)]
        right = jnp.concatenate(
            [jnp.where(hit, term, zero) for term in (one, part, rest) for hit in hits], axis=0
        )
        return magnitude, left, right, stats

    def count(lefts, rights):
        acc[...] += lax.dot_general(
            jnp.concatenate(lefts, axis=1), jnp.concatenate(rights, axis=1),
            (((1,), (1,)), ((), ())), preferred_element_type=jnp.float32,
        )

    def tiles(pairs, stats, fresh):
        lefts, rights = [], []
        for p, which in pairs:
            if fresh:
                out_x = jnp.zeros((8, dx), jnp.float32)
                out_yz = jnp.zeros((8, dx), jnp.float32)
            else:
                out_x, out_yz = rim_x[p], rim_yz[p]
            for j in which:
                z, y = 4 + 2 * p + j // 8, 8 + 8 * (j % 8)
                center = ext[z, pl.ds(y, 8), :]
                grad_x = grad_y = grad_z = None
                for k, coef in enumerate(COEF, start=1):
                    term_x = coef * (pltpu.roll(center, dx - k, 1) - pltpu.roll(center, k, 1))
                    term_y = coef * (ext[z, pl.ds(y + k, 8), :] - ext[z, pl.ds(y - k, 8), :])
                    term_z = coef * (ext[z + k, pl.ds(y, 8), :] - ext[z - k, pl.ds(y, 8), :])
                    grad_x = term_x if grad_x is None else grad_x + term_x
                    grad_y = term_y if grad_y is None else grad_y + term_y
                    grad_z = term_z if grad_z is None else grad_z + term_z
                square_yz = grad_z * grad_z + grad_y * grad_y
                out_x = jnp.where(slot == j, pltpu.roll(grad_x, 8 * j + 4, 1), out_x)
                out_yz = jnp.where(slot == j, pltpu.roll(square_yz, 8 * j + 4, 1), out_yz)
                magnitude, left, right, stats = classify(
                    square_yz + grad_x * grad_x, half_core, stats
                )
                mag_ref[2 * p + j // 8, pl.ds(8 * (j % 8), 8), :] = magnitude
                lefts.append(left)
                rights.append(right)
            rim_x[p] = out_x
            rim_yz[p] = out_yz
        count(lefts, rights)
        return stats

    inner = [j for j in range(16) if 0 < j % 8 < 7]
    outer = [j for j in range(16) if not 0 < j % 8 < 7]
    nothing = jnp.zeros((8, dx), jnp.float32)
    stats = (nothing, nothing, jnp.full((8, dx), 1e30, jnp.float32))

    stats = lax.fori_loop(
        0, (dz - 8) // 4,
        lambda i, s: tiles([(2 + 2 * i, inner), (3 + 2 * i, inner)], s, True), stats,
    )

    for copy in y_rims:
        copy.wait_send()
        copy.wait_recv()
    if ny > 4:
        signal(far2, c=-2)
        signal(far2, c=2)
    stats = lax.fori_loop(
        0, (dz - 8) // 8,
        lambda i, s: tiles([(2 + 4 * i + k, outer) for k in range(4)], s, False), stats,
    )

    for copy in xz_rims:
        copy.wait_send()
        copy.wait_recv()
    if ny > 4:
        pl.semaphore_wait(far2, 2)
        signal(far3, c=-4)
        signal(far3, c=4)
    if nz > 4:
        signal(near2, b=-2)
        signal(near2, b=2)
        signal(near2, a=2)
    stats = lax.fori_loop(
        0, 4,
        lambda i, s: tiles([(i + (dz // 2 - 4) * (i // 2), range(16))], s, True), stats,
    )
    if nz > 4:
        pl.semaphore_wait(near2, 3)
        signal(near3, b=4)

    rim_stats = (nothing, nothing, jnp.full((8, dx), 1e30, jnp.float32))

    def rims(i, rim_stats):
        lefts, rights = [], []
        for p in [8 * i + k for k in range(8)]:
            own = packed[p]
            high = jnp.where(left_rim, 0.0, from_high[p] - own)
            low = jnp.where(left_rim, from_low[p] - own, 0.0)
            fix_high = fix_low = None
            for k, coef in enumerate(COEF, start=1):
                more = coef * pltpu.roll(high, dx - k, 1)
                less = coef * pltpu.roll(low, k, 1)
                fix_high = more if fix_high is None else fix_high + more
                fix_low = less if fix_low is None else fix_low + less
            grad_x = rim_x[p] + jnp.where(left_rim, fix_high, -fix_low)
            magnitude, left, right, rim_stats = classify(
                rim_yz[p] + grad_x * grad_x, half, rim_stats
            )
            rim_x[p] = magnitude
            lefts.append(left)
            rights.append(right)
        count(lefts, rights)
        return rim_stats

    rim_stats = lax.fori_loop(0, dz // 16, rims, rim_stats)

    wsum = rim_stats[0] + jnp.where(rim_lane, 0.0, stats[0])
    wmax = jnp.maximum(rim_stats[1], jnp.where(rim_lane, 0.0, stats[1]))
    wmin = jnp.minimum(rim_stats[2], jnp.where(rim_lane, 1e30, stats[2]))

    total = acc[...]
    same = (
        lax.broadcasted_iota(jnp.int32, total.shape, 0) % 8
        == lax.broadcasted_iota(jnp.int32, total.shape, 1) % 8
    )
    total = jnp.where(same, total, 0.0).reshape(32, 8, 192).sum(axis=1)
    source = lax.broadcasted_iota(jnp.int32, (192, 128), 0)
    target = lax.broadcasted_iota(jnp.int32, (192, 128), 1)
    fits = (source // 8) % 8 == target % 8
    coarse_row = lax.broadcasted_iota(jnp.int32, (32, 128), 0)
    coarse_lane = lax.broadcasted_iota(jnp.int32, (32, 128), 1)
    keep = coarse_row % 16 == coarse_lane // 8

    def bins_of(chosen):
        spread = lax.dot_general(
            total, jnp.where(fits & chosen, 1.0, 0.0), (((1,), (0,)), ((), ())),
            precision=lax.Precision.HIGHEST, preferred_element_type=jnp.float32,
        )
        spread = jnp.where(keep, spread, 0.0)
        return spread[:16].sum(axis=0, keepdims=True), spread[16:].sum(axis=0, keepdims=True)

    number = bins_of(source < 64)
    part = bins_of(source >= 64)
    lane1 = lane[:1]
    turned = [pltpu.roll(pair(pair(pair(x))), 1, 1)[:1] for x in part]
    row0 = number[0] - part[0] + jnp.where(lane1 == 0, turned[1], turned[0])
    row1 = number[1] - part[1] + jnp.where(lane1 == 0, turned[0], turned[1])
    row2 = jnp.where(
        lane1 == 0, jnp.sum(wsum),
        jnp.where(lane1 == 1, jnp.max(wmax), jnp.min(wmin)),
    )
    msg[0:3, :] = jnp.concatenate([row0, row1, row2], axis=0)

    def merged(slots, slot_ref):
        value = slot_ref[0]
        added, most, least = value, value, value
        for k in range(1, slots):
            value = slot_ref[k]
            added, most, least = added + value, jnp.maximum(most, value), jnp.minimum(least, value)
        lane3 = lax.broadcasted_iota(jnp.int32, added.shape, 1)
        row3 = lax.broadcasted_iota(jnp.int32, added.shape, 0)
        return jnp.where(
            (row3 < 2) | (lane3 == 0), added, jnp.where(lane3 == 1, most, least)
        )

    def spread_out(peers, slot_ref, send_one, recv_one):
        slot_ref[0] = msg[...]
        for k, offset in enumerate(peers, start=1):
            pltpu.make_async_remote_copy(
                src_ref=msg, dst_ref=slot_ref.at[k], send_sem=send_one, recv_sem=recv_one,
                device_id=device(**offset), device_id_type=MESH,
            ).start()

    def gathered(slots, slot_ref, send_one, recv_one):
        rest = slot_ref.at[pl.ds(1, slots - 1)]
        pltpu.make_async_copy(rest, rest, send_one).wait()
        pltpu.make_async_copy(rest, rest, recv_one).wait()
        return merged(slots, slot_ref)

    def far(a, n):
        return min(a, n - a)

    plane_peers = sorted(
        [(a, b) for a in range(nx) for b in range(nz) if a or b],
        key=lambda ab: -(far(ab[0], nx) + far(ab[1], nz)),
    )
    line_peers = sorted(range(1, ny), key=lambda c: -far(c, ny))

    if nz > 4:
        pl.semaphore_wait(near3, 1)
    spread_out([dict(a=a, b=b) for a, b in plane_peers], plane, plane_send, plane_recv)

    def unpack(i, _):
        for p in (4 * i, 4 * i + 1, 4 * i + 2, 4 * i + 3):
            rim = rim_x[p]
            for j in range(16):
                at = (2 * p + j // 8, pl.ds(8 * (j % 8), 8))
                moved = pltpu.roll(rim, (dx - 8 * j - 4) % dx, 1)
                mag_ref[at] = jnp.where(rim_lane, moved, mag_ref[at])
        return 0

    lax.fori_loop(0, dz // 8, unpack, 0)

    msg[...] = gathered(nx * nz, plane, plane_send, plane_recv)
    if ny > 4:
        pl.semaphore_wait(far3, 2)
    spread_out([dict(c=c) for c in line_peers], line, line_send, line_recv)
    done = gathered(ny, line, line_send, line_recv)

    hist_ref[pl.ds(0, 128)] = done[0] * (BINS / cells)
    hist_ref[pl.ds(128, 128)] = done[1] * (BINS / cells)
    bin_id = lax.broadcasted_iota(jnp.int32, (2, 128), 0) * 128 + lax.broadcasted_iota(
        jnp.int32, (2, 128), 1
    )
    inside = (bin_id >= first[0]) & (bin_id < beyond[0])
    number = jnp.sum(jnp.where(inside, done[0:2], 0.0))
    last = done[2:3]
    total, most, least = (jnp.sum(jnp.where(lane1 == k, last, 0.0)) for k in range(3))
    stat_ref[0] = least
    stat_ref[1] = most
    stat_ref[2] = total * (1.0 / cells)
    stat_ref[3] = number * (1.0 / cells)


def solution(mesh):
    sizes = tuple(mesh.shape[name] for name in ("gx", "gy", "gz"))
    nx, ny, nz = sizes

    def on_device(u, first, beyond):
        dz, dy, dx = u.shape
        cells = u.size * nx * ny * nz
        rims = pltpu.VMEM((dz // 2, 8, dx), jnp.float32)
        return pl.pallas_call(
            functools.partial(kernel, sizes, cells),
            out_shape=(
                pltpu.VMEM(u.shape, jnp.float32),
                pltpu.VMEM((BINS,), jnp.float32),
                pltpu.SMEM((4,), jnp.float32),
            ),
            in_specs=[pl.BlockSpec(memory_space=pltpu.HBM)] * 3,
            out_specs=(
                pl.BlockSpec(memory_space=pltpu.VMEM),
                pl.BlockSpec(memory_space=pltpu.VMEM),
                pl.BlockSpec(memory_space=pltpu.SMEM),
            ),
            scratch_shapes=[
                pltpu.VMEM((dz + 8, dy + 16, dx), jnp.float32),
                rims, rims, rims, rims, rims,
                pltpu.VMEM((256, 192), jnp.float32),
                pltpu.VMEM((3, 128), jnp.float32),
                pltpu.VMEM((nx * nz, 3, 128), jnp.float32),
                pltpu.VMEM((ny, 3, 128), jnp.float32),
                pltpu.SMEM((1,), jnp.int32),
                pltpu.SMEM((1,), jnp.int32),
                pltpu.SemaphoreType.DMA,
                pltpu.SemaphoreType.DMA((2,)),
                pltpu.SemaphoreType.DMA((6,)),
                pltpu.SemaphoreType.DMA((6,)),
                pltpu.SemaphoreType.DMA,
                pltpu.SemaphoreType.DMA,
                pltpu.SemaphoreType.DMA,
                pltpu.SemaphoreType.DMA,
                pltpu.SemaphoreType.REGULAR,
                pltpu.SemaphoreType.REGULAR,
                pltpu.SemaphoreType.REGULAR,
                pltpu.SemaphoreType.REGULAR,
            ],
            compiler_params=pltpu.CompilerParams(collective_id=0, has_side_effects=True),
        )(u, first, beyond)

    return jax.shard_map(
        on_device,
        mesh=mesh,
        in_specs=(P("gz", "gy", "gx"), P(), P()),
        out_specs=(P("gz", "gy", "gx"), P(), P()),
        check_vma=False,
    )
```

```python
import functools

import jax
import jax.numpy as jnp
from jax import lax
from jax.experimental import pallas as pl
from jax.experimental.pallas import tpu as pltpu
from jax.sharding import PartitionSpec as P

MESH = pl.DeviceIdType.MESH
BINS = 256
RANGE = 12.0
SCALE = 0.8
COEF = (1.0, -1.0 / 4.0, 1.0 / 21.0, -1.0 / 224.0)


def pair(x):
    return jnp.concatenate([x, x], axis=0)


def kernel(
    sizes, cells, u_hbm, first_hbm, beyond_hbm, mag_ref, hist_ref, stat_ref,
    ext, packed, from_low, from_high, rim_x, rim_yz, acc, msg, plane, line, first, beyond,
    in_sem, edge_sem, send_sem, recv_sem, plane_send, plane_recv, line_send, line_recv,
    near2, near3, far2, far3,
):
    nx, ny, nz = sizes
    dz, dy, dx = u_hbm.shape
    gx, gy, gz = lax.axis_index("gx"), lax.axis_index("gy"), lax.axis_index("gz")

    def device(a=0, c=0, b=0):
        return {
            "gx": lax.rem(gx + (a + nx), nx) if a else gx,
            "gy": lax.rem(gy + (c + ny), ny) if c else gy,
            "gz": lax.rem(gz + (b + nz), nz) if b else gz,
        }

    def signal(sem, **offset):
        pl.semaphore_signal(sem, inc=1, device_id=device(**offset), device_id_type=MESH)

    loads = [
        pltpu.make_async_copy(
            u_hbm.at[pl.ds(z, 8)], ext.at[pl.ds(4 + z, 8), pl.ds(8, dy), :], in_sem.at[z // 8]
        )
        for z in range(0, dz, 8)
    ]
    for load in loads:
        load.start()
    barrier = pltpu.get_barrier_semaphore()
    for offset in (dict(a=-1), dict(a=1), dict(c=-1), dict(c=1), dict(b=-1), dict(b=1)):
        signal(barrier, **offset)
    edge_loads = [
        pltpu.make_async_copy(first_hbm, first, edge_sem.at[0]),
        pltpu.make_async_copy(beyond_hbm, beyond, edge_sem.at[1]),
    ]
    for copy in edge_loads:
        copy.start()

    lane = lax.broadcasted_iota(jnp.int32, (8, dx), 1)
    slot = lane // 8
    left_rim = lane % 8 < 4
    rim_lane = (lane < 4) | (lane >= dx - 4)
    top = jnp.full((8, dx), BINS - 2.0, jnp.float32)
    core_top = jnp.where(rim_lane, -32.0, top)
    spread = (lax.broadcasted_iota(jnp.int32, (8, dx), 0) * dx + lane) * 389 % 1024
    spread = (spread.astype(jnp.float32) + 0.5) * (1.0 / 1024.0)

    for i, load in enumerate(loads):
        load.wait()
        for p in range(4 * i, 4 * i + 4):
            out = jnp.zeros((8, dx), jnp.float32)
            for j in range(16):
                cell = ext[4 + 2 * p + j // 8, pl.ds(8 + 8 * (j % 8), 8), :]
                out = jnp.where(slot == j, pltpu.roll(cell, 8 * j + 4, 1), out)
            packed[p] = out

    pl.semaphore_wait(barrier, 6)

    def send(k, src, dst, **offset):
        copy = pltpu.make_async_remote_copy(
            src_ref=src, dst_ref=dst, send_sem=send_sem.at[k], recv_sem=recv_sem.at[k],
            device_id=device(**offset), device_id_type=MESH,
        )
        copy.start()
        return copy

    rows = pl.ds(8, dy)
    planes = pl.ds(4, dz)
    y_rims = [
        send(0, ext.at[planes, pl.ds(8, 4), :], ext.at[planes, pl.ds(8 + dy, 4), :], c=-1),
        send(1, ext.at[planes, pl.ds(4 + dy, 4), :], ext.at[planes, pl.ds(4, 4), :], c=1),
    ]
    xz_rims = [
        send(4, ext.at[pl.ds(4, 4), rows, :], ext.at[pl.ds(4 + dz, 4), rows, :], b=-1),
        send(5, ext.at[pl.ds(dz, 4), rows, :], ext.at[pl.ds(0, 4), rows, :], b=1),
        send(2, packed, from_high, a=-1),
        send(3, packed, from_low, a=1),
    ]
    acc[...] = jnp.zeros_like(acc)
    for copy in edge_loads:
        copy.wait()
    low_edge = first[0].astype(jnp.float32) - 1.0
    high_edge = beyond[0].astype(jnp.float32) - 1.0

    def classify(square, last, stats):
        wsum, wmax, wmin = stats
        root = square * (SCALE * SCALE) + 1.0
        magnitude = root * lax.rsqrt(root) - 1.0
        place = jnp.clip(magnitude * (BINS / RANGE) - 0.5, 0.0, BINS - 1.0)
        low = jnp.minimum(jnp.floor(place), last)
        share = jnp.floor((place - low) * 256.0 + spread)
        weight = jnp.clip(place - low_edge, 0.0, 1.0) - jnp.clip(place - high_edge, 0.0, 1.0)
        value = weight * magnitude
        stats = (
            wsum + value,
            jnp.maximum(wmax, value),
            jnp.minimum(wmin, magnitude - RANGE * weight),
        )
        coarse = jnp.floor(low * 0.0625)
        fine = low - 16.0 * coarse
        coarse = jnp.concatenate([coarse, coarse - 1.0], axis=0).astype(jnp.bfloat16)
        fine = jnp.concatenate([fine, fine - 1.0], axis=0).astype(jnp.bfloat16)
        share = pair(share).astype(jnp.bfloat16)
        one = jnp.ones((16, dx), jnp.bfloat16)
        zero = jnp.zeros((16, dx), jnp.bfloat16)
        coarse_hot = jnp.concatenate(
            [jnp.where(coarse == jnp.bfloat16(2 * k), one, zero) for k in range(8)], axis=0
        )
        hits = [fine == jnp.bfloat16(2 * k) for k in range(8)]
        fine_hot = jnp.concatenate(
            [jnp.where(hit, term, zero) for term in (one, share) for hit in hits], axis=0
        )
        return magnitude, fine_hot, coarse_hot, stats

    def count(fines, coarses):
        acc[...] += lax.dot_general(
            jnp.concatenate(coarses, axis=1), jnp.concatenate(fines, axis=1),
            (((1,), (1,)), ((), ())), preferred_element_type=jnp.float32,
        )

    def tiles(pairs, stats, fresh):
        fines, coarses = [], []
        for p, which in pairs:
            if fresh:
                out_x = jnp.zeros((8, dx), jnp.float32)
                out_yz = jnp.zeros((8, dx), jnp.float32)
            else:
                out_x, out_yz = rim_x[p], rim_yz[p]
            for j in which:
                z, y = 4 + 2 * p + j // 8, 8 + 8 * (j % 8)
                center = ext[z, pl.ds(y, 8), :]
                for k, coef in enumerate(COEF, start=1):
                    term_x = pltpu.roll(center, dx - k, 1) - pltpu.roll(center, k, 1)
                    term_y = ext[z, pl.ds(y + k, 8), :] - ext[z, pl.ds(y - k, 8), :]
                    term_z = ext[z + k, pl.ds(y, 8), :] - ext[z - k, pl.ds(y, 8), :]
                    grad_x = term_x if k == 1 else grad_x + coef * term_x
                    grad_y = term_y if k == 1 else grad_y + coef * term_y
                    grad_z = term_z if k == 1 else grad_z + coef * term_z
                square_yz = grad_z * grad_z + grad_y * grad_y
                out_x = jnp.where(slot == j, pltpu.roll(grad_x, 8 * j + 4, 1), out_x)
                out_yz = jnp.where(slot == j, pltpu.roll(square_yz, 8 * j + 4, 1), out_yz)
                magnitude, fine_hot, coarse_hot, stats = classify(
                    square_yz + grad_x * grad_x, core_top, stats
                )
                mag_ref[2 * p + j // 8, pl.ds(8 * (j % 8), 8), :] = magnitude
                fines.append(fine_hot)
                coarses.append(coarse_hot)
            rim_x[p] = out_x
            rim_yz[p] = out_yz
        count(fines, coarses)
        return stats

    inner = [j for j in range(16) if 0 < j % 8 < 7]
    outer = [j for j in range(16) if not 0 < j % 8 < 7]
    nothing = jnp.zeros((8, dx), jnp.float32)
    stats = (nothing, nothing, jnp.full((8, dx), 1e30, jnp.float32))

    stats = lax.fori_loop(
        0, (dz - 8) // 8,
        lambda i, s: tiles([(2 + 4 * i + k, inner) for k in range(4)], s, True), stats,
    )

    for copy in y_rims:
        copy.wait_send()
        copy.wait_recv()
    if ny > 4:
        signal(far2, c=-2)
        signal(far2, c=2)
    stats = lax.fori_loop(
        0, 2,
        lambda i, s: tiles(
            [(2 + (dz - 8) // 4 * i + k, outer) for k in range((dz - 8) // 4)], s, False
        ), stats,
    )

    for copy in xz_rims:
        copy.wait_send()
        copy.wait_recv()
    if ny > 4:
        pl.semaphore_wait(far2, 2)
        signal(far3, c=-4)
        signal(far3, c=4)
    if nz > 4:
        signal(near2, b=-2)
        signal(near2, b=2)
        signal(near2, a=2)
    stats = lax.fori_loop(
        0, 2,
        lambda i, s: tiles([(k + (dz // 2 - 2) * i, range(16)) for k in range(2)], s, True), stats,
    )
    if nz > 4:
        pl.semaphore_wait(near2, 3)
        signal(near3, b=4)

    rim_stats = (nothing, nothing, jnp.full((8, dx), 1e30, jnp.float32))

    fines, coarses = [], []
    for p in range(dz // 2):
        own = packed[p]
        high = jnp.where(left_rim, 0.0, from_high[p] - own)
        low = jnp.where(left_rim, from_low[p] - own, 0.0)
        fix_high = fix_low = None
        for k, coef in enumerate(COEF, start=1):
            more = coef * pltpu.roll(high, dx - k, 1)
            less = coef * pltpu.roll(low, k, 1)
            fix_high = more if fix_high is None else fix_high + more
            fix_low = less if fix_low is None else fix_low + less
        grad_x = rim_x[p] + jnp.where(left_rim, fix_high, -fix_low)
        magnitude, fine_hot, coarse_hot, rim_stats = classify(rim_yz[p] + grad_x * grad_x, top, rim_stats)
        rim_x[p] = magnitude
        fines.append(fine_hot)
        coarses.append(coarse_hot)
    count(fines, coarses)

    wsum = rim_stats[0] + jnp.where(rim_lane, 0.0, stats[0])
    wmax = jnp.maximum(rim_stats[1], jnp.where(rim_lane, 0.0, stats[1]))
    wmin = jnp.minimum(rim_stats[2], jnp.where(rim_lane, 1e30, stats[2]))

    total = acc[...]
    same = (
        lax.broadcasted_iota(jnp.int32, total.shape, 0) % 8
        == lax.broadcasted_iota(jnp.int32, total.shape, 1) % 8
    )
    total = jnp.where(same, total, 0.0).reshape(16, 8, 256).sum(axis=1)
    source = lax.broadcasted_iota(jnp.int32, (256, 256), 0)
    target = lax.broadcasted_iota(jnp.int32, (256, 256), 1)
    fits = (source // 128 == target // 128) & ((source // 8) % 16 == target % 16)
    total = lax.dot_general(
        total, jnp.where(fits, 1.0, 0.0), (((1,), (0,)), ((), ())),
        precision=lax.Precision.HIGHEST, preferred_element_type=jnp.float32,
    )
    keep = (
        lax.broadcasted_iota(jnp.int32, (16, 256), 0) % 8
        == (lax.broadcasted_iota(jnp.int32, (16, 256), 1) % 128) // 16
    )
    total = jnp.where(keep, total, 0.0)
    halves = [x.sum(axis=0, keepdims=True) for x in (total[:8], total[8:])]
    number = [x[:, :128] for x in halves]
    part = [x[:, 128:] * (1.0 / 256.0) for x in halves]
    lane1 = lane[:1]
    turned = [pltpu.roll(pair(pair(pair(x))), 1, 1)[:1] for x in part]
    row0 = number[0] - part[0] + jnp.where(lane1 == 0, turned[1], turned[0])
    row1 = number[1] - part[1] + jnp.where(lane1 == 0, turned[0], turned[1])
    row2 = jnp.where(
        lane1 == 0, jnp.sum(wsum),
        jnp.where(lane1 == 1, jnp.max(wmax), jnp.min(wmin) + RANGE),
    )
    msg[0:3, :] = jnp.concatenate([row0, row1, row2], axis=0)

    def merged(slots, slot_ref):
        value = slot_ref[0]
        added, most, least = value, value, value
        for k in range(1, slots):
            value = slot_ref[k]
            added, most, least = added + value, jnp.maximum(most, value), jnp.minimum(least, value)
        lane3 = lax.broadcasted_iota(jnp.int32, added.shape, 1)
        row3 = lax.broadcasted_iota(jnp.int32, added.shape, 0)
        return jnp.where(
            (row3 < 2) | (lane3 == 0), added, jnp.where(lane3 == 1, most, least)
        )

    def spread_out(peers, slot_ref, send_one, recv_one):
        slot_ref[0] = msg[...]
        for k, offset in enumerate(peers, start=1):
            pltpu.make_async_remote_copy(
                src_ref=msg, dst_ref=slot_ref.at[k], send_sem=send_one, recv_sem=recv_one,
                device_id=device(**offset), device_id_type=MESH,
            ).start()

    def gathered(slots, slot_ref, send_one, recv_one):
        rest = slot_ref.at[pl.ds(1, slots - 1)]
        pltpu.make_async_copy(rest, rest, send_one).wait()
        pltpu.make_async_copy(rest, rest, recv_one).wait()
        return merged(slots, slot_ref)

    def far(a, n):
        return min(a, n - a)

    plane_peers = sorted(
        [(a, b) for a in range(nx) for b in range(nz) if a or b],
        key=lambda ab: -(far(ab[0], nx) + far(ab[1], nz)),
    )
    line_peers = sorted(range(1, ny), key=lambda c: -far(c, ny))

    if nz > 4:
        pl.semaphore_wait(near3, 1)
    spread_out([dict(a=a, b=b) for a, b in plane_peers], plane, plane_send, plane_recv)

    def unpack(i, _):
        for p in (4 * i, 4 * i + 1, 4 * i + 2, 4 * i + 3):
            rim = rim_x[p]
            for j in range(16):
                at = (2 * p + j // 8, pl.ds(8 * (j % 8), 8))
                moved = pltpu.roll(rim, (dx - 8 * j - 4) % dx, 1)
                mag_ref[at] = jnp.where(rim_lane, moved, mag_ref[at])
        return 0

    lax.fori_loop(0, dz // 8, unpack, 0)

    msg[...] = gathered(nx * nz, plane, plane_send, plane_recv)
    if ny > 4:
        pl.semaphore_wait(far3, 2)
    spread_out([dict(c=c) for c in line_peers], line, line_send, line_recv)
    done = gathered(ny, line, line_send, line_recv)

    hist_ref[pl.ds(0, 128)] = done[0] * (BINS / cells)
    hist_ref[pl.ds(128, 128)] = done[1] * (BINS / cells)
    bin_id = lax.broadcasted_iota(jnp.int32, (2, 128), 0) * 128 + lax.broadcasted_iota(
        jnp.int32, (2, 128), 1
    )
    inside = (bin_id >= first[0]) & (bin_id < beyond[0])
    number = jnp.sum(jnp.where(inside, done[0:2], 0.0))
    last = done[2:3]
    total, most, least = (jnp.sum(jnp.where(lane1 == k, last, 0.0)) for k in range(3))
    stat_ref[0] = least
    stat_ref[1] = most
    stat_ref[2] = total * (1.0 / cells)
    stat_ref[3] = number * (1.0 / cells)


def write_out(mag, hist, stat, mag_hbm, hist_hbm, stat_hbm, sems):
    step = mag.shape[0] // 4
    copies = [
        pltpu.make_async_copy(hist, hist_hbm, sems.at[0]),
        pltpu.make_async_copy(stat, stat_hbm, sems.at[1]),
    ]
    for k in range(4):
        part = pl.ds(step * k, step)
        copies.append(pltpu.make_async_copy(mag.at[part], mag_hbm.at[part], sems.at[2 + k]))
    for copy in copies:
        copy.start()
    for copy in copies:
        copy.wait()


def solution(mesh):
    sizes = tuple(mesh.shape[name] for name in ("gx", "gy", "gz"))
    nx, ny, nz = sizes

    def on_device(u, first, beyond):
        dz, dy, dx = u.shape
        cells = u.size * nx * ny * nz
        rims = pltpu.VMEM((dz // 2, 8, dx), jnp.float32)
        mag, hist, stat = pl.pallas_call(
            functools.partial(kernel, sizes, cells),
            out_shape=(
                pltpu.VMEM(u.shape, jnp.float32),
                pltpu.VMEM((BINS,), jnp.float32),
                pltpu.SMEM((4,), jnp.float32),
            ),
            in_specs=[pl.BlockSpec(memory_space=pltpu.HBM)] * 3,
            out_specs=(
                pl.BlockSpec(memory_space=pltpu.VMEM),
                pl.BlockSpec(memory_space=pltpu.VMEM),
                pl.BlockSpec(memory_space=pltpu.SMEM),
            ),
            scratch_shapes=[
                pltpu.VMEM((dz + 8, dy + 16, dx), jnp.float32),
                rims, rims, rims, rims, rims,
                pltpu.VMEM((128, 256), jnp.float32),
                pltpu.VMEM((3, 128), jnp.float32),
                pltpu.VMEM((nx * nz, 3, 128), jnp.float32),
                pltpu.VMEM((ny, 3, 128), jnp.float32),
                pltpu.SMEM((1,), jnp.int32),
                pltpu.SMEM((1,), jnp.int32),
                pltpu.SemaphoreType.DMA((dz // 8,)),
                pltpu.SemaphoreType.DMA((2,)),
                pltpu.SemaphoreType.DMA((6,)),
                pltpu.SemaphoreType.DMA((6,)),
                pltpu.SemaphoreType.DMA,
                pltpu.SemaphoreType.DMA,
                pltpu.SemaphoreType.DMA,
                pltpu.SemaphoreType.DMA,
                pltpu.SemaphoreType.REGULAR,
                pltpu.SemaphoreType.REGULAR,
                pltpu.SemaphoreType.REGULAR,
                pltpu.SemaphoreType.REGULAR,
            ],
            compiler_params=pltpu.CompilerParams(collective_id=0, has_side_effects=True),
        )(u, first, beyond)
        mag = pltpu.with_memory_space_constraint(mag, pltpu.VMEM)
        hist = pltpu.with_memory_space_constraint(hist, pltpu.VMEM)
        return pl.pallas_call(
            write_out,
            out_shape=(
                jax.ShapeDtypeStruct(u.shape, jnp.float32),
                jax.ShapeDtypeStruct((BINS,), jnp.float32),
                jax.ShapeDtypeStruct((4,), jnp.float32),
            ),
            in_specs=[
                pl.BlockSpec(memory_space=pltpu.VMEM),
                pl.BlockSpec(memory_space=pltpu.VMEM),
                pl.BlockSpec(memory_space=pltpu.SMEM),
            ],
            out_specs=[pl.BlockSpec(memory_space=pltpu.HBM)] * 3,
            scratch_shapes=[pltpu.SemaphoreType.DMA((6,))],
        )(mag, hist, stat)

    return jax.shard_map(
        on_device,
        mesh=mesh,
        in_specs=(P("gz", "gy", "gx"), P(), P()),
        out_specs=(P("gz", "gy", "gx"), P(), P()),
        check_vma=False,
    )
```

```python
import functools

import jax
import jax.numpy as jnp
from jax import lax
from jax.experimental import pallas as pl
from jax.experimental.pallas import tpu as pltpu
from jax.sharding import PartitionSpec as P

MESH = pl.DeviceIdType.MESH
BINS = 256
RANGE = 12.0
SCALE = 0.8
COEF = (1.0, -1.0 / 4.0, 1.0 / 21.0, -1.0 / 224.0)


def pair(x):
    return jnp.concatenate([x, x], axis=0)


def kernel(
    sizes, cells, u_hbm, first_hbm, beyond_hbm, mag_ref, hist_ref, stat_ref,
    ext, packed, to_low, to_high, from_low, from_high, rim_x, rim_yz, acc, msg, plane, line, first, beyond,
    in_sem, edge_sem, send_sem, recv_sem, plane_send, plane_recv, line_send, line_recv,
    hop1, near2, near3, far2, far3,
):
    nx, ny, nz = sizes
    dz, dy, dx = u_hbm.shape
    gx, gy, gz = lax.axis_index("gx"), lax.axis_index("gy"), lax.axis_index("gz")

    def device(a=0, c=0, b=0):
        return {
            "gx": lax.rem(gx + (a + nx), nx) if a else gx,
            "gy": lax.rem(gy + (c + ny), ny) if c else gy,
            "gz": lax.rem(gz + (b + nz), nz) if b else gz,
        }

    def signal(sem, **offset):
        pl.semaphore_signal(sem, inc=1, device_id=device(**offset), device_id_type=MESH)

    loads = [
        pltpu.make_async_copy(
            u_hbm.at[pl.ds(z, 8)], ext.at[pl.ds(4 + z, 8), pl.ds(8, dy), :], in_sem.at[z // 8]
        )
        for z in sorted(range(0, dz, 8), key=lambda z: min(z, dz - 8 - z))
    ]
    for load in loads:
        load.start()
    barrier = pltpu.get_barrier_semaphore()
    neighbours = (dict(a=-1), dict(a=1), dict(b=-1), dict(b=1), dict(c=-1), dict(c=1))
    for offset in neighbours:
        signal(barrier, **offset)
    edge_loads = [
        pltpu.make_async_copy(first_hbm, first, edge_sem.at[0]),
        pltpu.make_async_copy(beyond_hbm, beyond, edge_sem.at[1]),
    ]
    for copy in edge_loads:
        copy.start()

    lane = lax.broadcasted_iota(jnp.int32, (8, dx), 1)
    slot = lane // 8
    left_rim = lane % 8 < 4
    rim_lane = (lane < 4) | (lane >= dx - 4)
    top = jnp.full((8, dx), BINS // 2 - 1.0, jnp.float32)
    core_top = jnp.where(rim_lane, -64.0, top)
    spread = (lax.broadcasted_iota(jnp.int32, (8, dx), 0) * dx + lane) * 389 % 1024
    spread = (spread.astype(jnp.float32) + 0.5) * (1.0 / 1024.0)

    def send(k, src, dst, **offset):
        copy = pltpu.make_async_remote_copy(
            src_ref=src, dst_ref=dst, send_sem=send_sem.at[k], recv_sem=recv_sem.at[k],
            device_id=device(**offset), device_id_type=MESH,
        )
        copy.start()
        return copy

    rows = pl.ds(8, dy)
    planes = pl.ds(4, dz)
    for load in loads[:2]:
        load.wait()
    pl.semaphore_wait(barrier, 6)
    z_rims = [
        send(0, ext.at[pl.ds(4, 4), rows, :], ext.at[pl.ds(4 + dz, 4), rows, :], b=-1),
        send(1, ext.at[pl.ds(dz, 4), rows, :], ext.at[pl.ds(0, 4), rows, :], b=1),
    ]
    for load in loads[2:]:
        load.wait()
    y_rims = [
        send(2, ext.at[planes, pl.ds(8, 4), :], ext.at[planes, pl.ds(8 + dy, 4), :], c=-1),
        send(3, ext.at[planes, pl.ds(4 + dy, 4), :], ext.at[planes, pl.ds(4, 4), :], c=1),
    ]
    for offset in neighbours:
        signal(hop1, **offset)
    for m in range(dz // 4):
        both = []
        for p in (2 * m, 2 * m + 1):
            out = jnp.zeros((8, dx), jnp.float32)
            for j in range(16):
                cell = ext[4 + 2 * p + j // 8, pl.ds(8 + 8 * (j % 8), 8), :]
                out = jnp.where(slot == j, pltpu.roll(cell, 8 * j + 4, 1), out)
            packed[p] = out
            both.append(out)
        to_high[m] = jnp.where(left_rim, both[0], pltpu.roll(both[1], 4, 1))
        to_low[m] = jnp.where(left_rim, pltpu.roll(both[0], dx - 4, 1), both[1])
    x_rims = [
        send(4, to_low, from_high, a=-1),
        send(5, to_high, from_low, a=1),
    ]
    acc[...] = jnp.zeros_like(acc)
    for copy in edge_loads:
        copy.wait()
    low_edge = first[0].astype(jnp.float32) * 0.5 - 0.5
    high_edge = beyond[0].astype(jnp.float32) * 0.5 - 0.5

    def classify(square, last, stats):
        wsum, wmax, wmin = stats
        root = square * (SCALE * SCALE) + 1.0
        magnitude = root * lax.rsqrt(root) - 1.0
        place = jnp.clip(magnitude * (0.5 * BINS / RANGE) - 0.25, 0.0, 0.5 * BINS - 0.5)
        low = jnp.minimum(jnp.floor(place), last)
        share = jnp.floor((place - low) * 512.0 + spread)
        weight = jnp.clip(place - low_edge, 0.0, 0.5) - jnp.clip(place - high_edge, 0.0, 0.5)
        value = weight * magnitude
        stats = (
            wsum + value,
            jnp.maximum(wmax, value),
            jnp.minimum(wmin, magnitude - (2.0 * RANGE) * weight),
        )
        coarse = jnp.floor(low * 0.125)
        fine = low - 8.0 * coarse
        coarse = jnp.concatenate([coarse, coarse - 1.0], axis=0).astype(jnp.bfloat16)
        fine = pair(fine).astype(jnp.bfloat16)
        here = jnp.concatenate(
            [jnp.maximum(256.0 - share, 0.0), jnp.minimum(share, 512.0 - share)], axis=0
        ).astype(jnp.bfloat16)
        after = jnp.concatenate(
            [jnp.maximum(share - 256.0, 0.0), jnp.zeros((8, dx), jnp.float32)], axis=0
        ).astype(jnp.bfloat16)
        one = jnp.ones((16, dx), jnp.bfloat16)
        zero = jnp.zeros((16, dx), jnp.bfloat16)
        coarse_hot = jnp.concatenate(
            [jnp.where(coarse == jnp.bfloat16(2 * k), one, zero) for k in range(8)], axis=0
        )
        hits = [fine == jnp.bfloat16(k) for k in range(8)]
        parts = [jnp.where(hits[0], here, zero)]
        for k in range(1, 8):
            parts.append(jnp.where(hits[k], here, jnp.where(hits[k - 1], after, zero)))
        parts.append(jnp.where(hits[7], after, zero))
        return magnitude, jnp.concatenate(parts, axis=0), coarse_hot, stats

    def count(fines, coarses):
        acc[...] += lax.dot_general(
            jnp.concatenate(coarses, axis=1), jnp.concatenate(fines, axis=1),
            (((1,), (1,)), ((), ())), preferred_element_type=jnp.float32,
        )

    def tiles(pairs, stats, fresh):
        fines, coarses = [], []
        for p, which in pairs:
            if fresh:
                out_x = jnp.zeros((8, dx), jnp.float32)
                out_yz = jnp.zeros((8, dx), jnp.float32)
            else:
                out_x, out_yz = rim_x[p], rim_yz[p]
            for j in which:
                z, y = 4 + 2 * p + j // 8, 8 + 8 * (j % 8)
                center = ext[z, pl.ds(y, 8), :]
                for k, coef in enumerate(COEF, start=1):
                    term_x = pltpu.roll(center, dx - k, 1) - pltpu.roll(center, k, 1)
                    term_y = ext[z, pl.ds(y + k, 8), :] - ext[z, pl.ds(y - k, 8), :]
                    term_z = ext[z + k, pl.ds(y, 8), :] - ext[z - k, pl.ds(y, 8), :]
                    grad_x = term_x if k == 1 else grad_x + coef * term_x
                    grad_y = term_y if k == 1 else grad_y + coef * term_y
                    grad_z = term_z if k == 1 else grad_z + coef * term_z
                square_yz = grad_z * grad_z + grad_y * grad_y
                out_x = jnp.where(slot == j, pltpu.roll(grad_x, 8 * j + 4, 1), out_x)
                out_yz = jnp.where(slot == j, pltpu.roll(square_yz, 8 * j + 4, 1), out_yz)
                magnitude, fine_hot, coarse_hot, stats = classify(
                    square_yz + grad_x * grad_x, core_top, stats
                )
                mag_ref[2 * p + j // 8, pl.ds(8 * (j % 8), 8), :] = magnitude
                fines.append(fine_hot)
                coarses.append(coarse_hot)
            rim_x[p] = out_x
            rim_yz[p] = out_yz
        count(fines, coarses)
        return stats

    inner = [j for j in range(16) if 0 < j % 8 < 7]
    outer = [j for j in range(16) if not 0 < j % 8 < 7]
    nothing = jnp.zeros((8, dx), jnp.float32)
    stats = (nothing, nothing, jnp.full((8, dx), 1e30, jnp.float32))

    def trips(count_of, pairs, which, stats, fresh):
        step = len(pairs) // count_of
        if count_of == 1:
            return tiles([(p, which) for p in pairs], stats, fresh)
        gap = pairs[step] - pairs[0]
        return lax.fori_loop(
            0, count_of, lambda i, s: tiles([(p + gap * i, which) for p in pairs[:step]], s, fresh), stats
        )

    middle = list(range(2, dz // 2 - 2))
    ends = [0, 1, dz // 2 - 2, dz // 2 - 1]

    stats = trips(3, middle, inner, stats, True)

    pl.semaphore_wait(hop1, 6)
    if nz > 4:
        signal(near2, b=-2)
        signal(near2, b=2)
        signal(near2, a=2)
    if ny > 4:
        signal(far2, c=-2)
        signal(far2, c=2)

    for copy in y_rims:
        copy.wait_send()
        copy.wait_recv()
    stats = trips(1, middle, outer, stats, False)

    for copy in z_rims:
        copy.wait_send()
        copy.wait_recv()
    stats = trips(2, ends, list(range(16)), stats, True)

    if nz > 4:
        pl.semaphore_wait(near2, 3)
        signal(near3, b=4)
    if ny > 4:
        pl.semaphore_wait(far2, 2)
        signal(far3, c=-4)
        signal(far3, c=4)

    rim_stats = (nothing, nothing, jnp.full((8, dx), 1e30, jnp.float32))

    for copy in x_rims:
        copy.wait_send()
        copy.wait_recv()
    fines, coarses = [], []
    for p in range(dz // 2):
        own = packed[p]
        high, low = from_high[p // 2], from_low[p // 2]
        if p % 2:
            low = pltpu.roll(low, dx - 4, 1)
        else:
            high = pltpu.roll(high, 4, 1)
        high = jnp.where(left_rim, 0.0, high - own)
        low = jnp.where(left_rim, low - own, 0.0)
        fix_high = fix_low = None
        for k, coef in enumerate(COEF, start=1):
            more = coef * pltpu.roll(high, dx - k, 1)
            less = coef * pltpu.roll(low, k, 1)
            fix_high = more if fix_high is None else fix_high + more
            fix_low = less if fix_low is None else fix_low + less
        grad_x = rim_x[p] + jnp.where(left_rim, fix_high, -fix_low)
        magnitude, fine_hot, coarse_hot, rim_stats = classify(rim_yz[p] + grad_x * grad_x, top, rim_stats)
        rim_x[p] = magnitude
        fines.append(fine_hot)
        coarses.append(coarse_hot)
    count(fines, coarses)

    wsum = rim_stats[0] + jnp.where(rim_lane, 0.0, stats[0])
    wmax = jnp.maximum(rim_stats[1], jnp.where(rim_lane, 0.0, stats[1]))
    wmin = jnp.minimum(rim_stats[2], jnp.where(rim_lane, 1e30, stats[2]))

    total = acc[...]
    same = (
        lax.broadcasted_iota(jnp.int32, total.shape, 0) % 8
        == lax.broadcasted_iota(jnp.int32, total.shape, 1) % 8
    )
    total = jnp.where(same, total, 0.0).reshape(16, 8, 144).sum(axis=1)
    source = lax.broadcasted_iota(jnp.int32, (144, 256), 0) // 8
    target = lax.broadcasted_iota(jnp.int32, (144, 256), 1)
    fits = (source == target % 16 + 16 * (target // 128)).astype(jnp.float32).astype(jnp.bfloat16)
    pieces = []
    for _ in range(3):
        pieces.append(total.astype(jnp.bfloat16))
        total = total - pieces[-1].astype(jnp.float32)
    total = lax.dot_general(
        jnp.concatenate(pieces, axis=0), fits, (((1,), (0,)), ((), ())),
        preferred_element_type=jnp.float32,
    )
    total = total[:16] + total[16:32] + total[32:]
    owner = lax.broadcasted_iota(jnp.int32, (16, 128), 1) // 16
    coarse = lax.broadcasted_iota(jnp.int32, (16, 128), 0)

    def bin_row(r):
        mine = jnp.where(coarse == owner + 8 * r, total[:, :128], 0.0)
        carried = jnp.where(coarse + 1 == owner + 8 * r, total[:, 128:], 0.0)
        return (mine + carried).sum(axis=0, keepdims=True) * (1.0 / 256.0)

    row0, row1 = bin_row(0), bin_row(1)
    lane1 = lane[:1]
    row2 = jnp.where(
        lane1 == 0, jnp.sum(wsum) * 2.0,
        jnp.where(lane1 == 1, jnp.max(wmax) * 2.0, jnp.min(wmin) + RANGE),
    )
    msg[0:3, :] = jnp.concatenate([row0, row1, row2], axis=0)

    def merged(slots, slot_ref):
        value = slot_ref[0]
        added, most, least = value, value, value
        for k in range(1, slots):
            value = slot_ref[k]
            added, most, least = added + value, jnp.maximum(most, value), jnp.minimum(least, value)
        lane3 = lax.broadcasted_iota(jnp.int32, added.shape, 1)
        row3 = lax.broadcasted_iota(jnp.int32, added.shape, 0)
        return jnp.where(
            (row3 < 2) | (lane3 == 0), added, jnp.where(lane3 == 1, most, least)
        )

    def spread_out(peers, slot_ref, send_one, recv_one):
        slot_ref[0] = msg[...]
        for k, offset in enumerate(peers, start=1):
            pltpu.make_async_remote_copy(
                src_ref=msg, dst_ref=slot_ref.at[k], send_sem=send_one, recv_sem=recv_one,
                device_id=device(**offset), device_id_type=MESH,
            ).start()

    def gathered(slots, slot_ref, send_one, recv_one):
        rest = slot_ref.at[pl.ds(1, slots - 1)]
        pltpu.make_async_copy(rest, rest, send_one).wait()
        pltpu.make_async_copy(rest, rest, recv_one).wait()
        return merged(slots, slot_ref)

    def far(a, n):
        return min(a, n - a)

    plane_peers = sorted(
        [(a, b) for a in range(nx) for b in range(nz) if a or b],
        key=lambda ab: -(far(ab[0], nx) + far(ab[1], nz)),
    )
    line_peers = sorted(range(1, ny), key=lambda c: -far(c, ny))

    if nz > 4:
        pl.semaphore_wait(near3, 1)
    spread_out([dict(a=a, b=b) for a, b in plane_peers], plane, plane_send, plane_recv)

    def unpack(i, _):
        for p in (4 * i, 4 * i + 1, 4 * i + 2, 4 * i + 3):
            rim = rim_x[p]
            for j in range(16):
                at = (2 * p + j // 8, pl.ds(8 * (j % 8), 8))
                moved = pltpu.roll(rim, (dx - 8 * j - 4) % dx, 1)
                mag_ref[at] = jnp.where(rim_lane, moved, mag_ref[at])
        return 0

    lax.fori_loop(0, dz // 8, unpack, 0)

    msg[...] = gathered(nx * nz, plane, plane_send, plane_recv)
    if ny > 4:
        pl.semaphore_wait(far3, 2)
    spread_out([dict(c=c) for c in line_peers], line, line_send, line_recv)
    done = gathered(ny, line, line_send, line_recv)

    hist_ref[pl.ds(0, 128)] = done[0] * (BINS / cells)
    hist_ref[pl.ds(128, 128)] = done[1] * (BINS / cells)
    bin_id = lax.broadcasted_iota(jnp.int32, (2, 128), 0) * 128 + lax.broadcasted_iota(
        jnp.int32, (2, 128), 1
    )
    inside = (bin_id >= first[0]) & (bin_id < beyond[0])
    number = jnp.sum(jnp.where(inside, done[0:2], 0.0))
    last = done[2:3]
    total, most, least = (jnp.sum(jnp.where(lane1 == k, last, 0.0)) for k in range(3))
    stat_ref[0] = least
    stat_ref[1] = most
    stat_ref[2] = total * (1.0 / cells)
    stat_ref[3] = number * (1.0 / cells)


def write_out(mag, hist, stat, mag_hbm, hist_hbm, stat_hbm, sems):
    step = mag.shape[0] // 4
    copies = [
        pltpu.make_async_copy(hist, hist_hbm, sems.at[0]),
        pltpu.make_async_copy(stat, stat_hbm, sems.at[1]),
    ]
    for k in range(4):
        part = pl.ds(step * k, step)
        copies.append(pltpu.make_async_copy(mag.at[part], mag_hbm.at[part], sems.at[2 + k]))
    for copy in copies:
        copy.start()
    for copy in copies:
        copy.wait()


def solution(mesh):
    sizes = tuple(mesh.shape[name] for name in ("gx", "gy", "gz"))
    nx, ny, nz = sizes

    def on_device(u, first, beyond):
        dz, dy, dx = u.shape
        cells = u.size * nx * ny * nz
        rims = pltpu.VMEM((dz // 2, 8, dx), jnp.float32)
        half_rims = pltpu.VMEM((dz // 4, 8, dx), jnp.float32)
        mag, hist, stat = pl.pallas_call(
            functools.partial(kernel, sizes, cells),
            out_shape=(
                pltpu.VMEM(u.shape, jnp.float32),
                pltpu.VMEM((BINS,), jnp.float32),
                pltpu.SMEM((4,), jnp.float32),
            ),
            in_specs=[pl.BlockSpec(memory_space=pltpu.HBM)] * 3,
            out_specs=(
                pl.BlockSpec(memory_space=pltpu.VMEM),
                pl.BlockSpec(memory_space=pltpu.VMEM),
                pl.BlockSpec(memory_space=pltpu.SMEM),
            ),
            scratch_shapes=[
                pltpu.VMEM((dz + 8, dy + 16, dx), jnp.float32),
                rims, half_rims, half_rims, half_rims, half_rims, rims, rims,
                pltpu.VMEM((128, 144), jnp.float32),
                pltpu.VMEM((3, 128), jnp.float32),
                pltpu.VMEM((nx * nz, 3, 128), jnp.float32),
                pltpu.VMEM((ny, 3, 128), jnp.float32),
                pltpu.SMEM((1,), jnp.int32),
                pltpu.SMEM((1,), jnp.int32),
                pltpu.SemaphoreType.DMA((dz // 8,)),
                pltpu.SemaphoreType.DMA((2,)),
                pltpu.SemaphoreType.DMA((6,)),
                pltpu.SemaphoreType.DMA((6,)),
                pltpu.SemaphoreType.DMA,
                pltpu.SemaphoreType.DMA,
                pltpu.SemaphoreType.DMA,
                pltpu.SemaphoreType.DMA,
                pltpu.SemaphoreType.REGULAR,
                pltpu.SemaphoreType.REGULAR,
                pltpu.SemaphoreType.REGULAR,
                pltpu.SemaphoreType.REGULAR,
                pltpu.SemaphoreType.REGULAR,
            ],
            compiler_params=pltpu.CompilerParams(collective_id=0, has_side_effects=True),
        )(u, first, beyond)
        mag = pltpu.with_memory_space_constraint(mag, pltpu.VMEM)
        hist = pltpu.with_memory_space_constraint(hist, pltpu.VMEM)
        return pl.pallas_call(
            write_out,
            out_shape=(
                jax.ShapeDtypeStruct(u.shape, jnp.float32),
                jax.ShapeDtypeStruct((BINS,), jnp.float32),
                jax.ShapeDtypeStruct((4,), jnp.float32),
            ),
            in_specs=[
                pl.BlockSpec(memory_space=pltpu.VMEM),
                pl.BlockSpec(memory_space=pltpu.VMEM),
                pl.BlockSpec(memory_space=pltpu.SMEM),
            ],
            out_specs=[pl.BlockSpec(memory_space=pltpu.HBM)] * 3,
            scratch_shapes=[pltpu.SemaphoreType.DMA((6,))],
        )(mag, hist, stat)

    return jax.shard_map(
        on_device,
        mesh=mesh,
        in_specs=(P("gz", "gy", "gx"), P(), P()),
        out_specs=(P("gz", "gy", "gx"), P(), P()),
        check_vma=False,
    )
```

```python
import functools

import jax
import jax.numpy as jnp
from jax import lax
from jax.experimental import pallas as pl
from jax.experimental.pallas import tpu as pltpu
from jax.sharding import PartitionSpec as P

MESH = pl.DeviceIdType.MESH
BINS = 256
RANGE = 12.0
SCALE = 0.8
COEF = (1.0, -1.0 / 4.0, 1.0 / 21.0, -1.0 / 224.0)


def pair(x):
    return jnp.concatenate([x, x], axis=0)


def kernel(
    sizes, cells, u_hbm, first_hbm, beyond_hbm, mag_ref, hist_ref, stat_ref,
    ext, packed, to_low, to_high, from_low, from_high, rim_x, rim_yz, acc, msg, plane, line, first, beyond,
    in_sem, edge_sem, send_sem, recv_sem, plane_send, plane_recv, line_send, line_recv,
    hop1, near2, near3, far2, far3,
):
    nx, ny, nz = sizes
    dz, dy, dx = u_hbm.shape
    gx, gy, gz = lax.axis_index("gx"), lax.axis_index("gy"), lax.axis_index("gz")

    def device(a=0, c=0, b=0):
        return {
            "gx": lax.rem(gx + (a + nx), nx) if a else gx,
            "gy": lax.rem(gy + (c + ny), ny) if c else gy,
            "gz": lax.rem(gz + (b + nz), nz) if b else gz,
        }

    def signal(sem, **offset):
        pl.semaphore_signal(sem, inc=1, device_id=device(**offset), device_id_type=MESH)

    loads = [
        pltpu.make_async_copy(
            u_hbm.at[pl.ds(z, 8)], ext.at[pl.ds(4 + z, 8), pl.ds(8, dy), :], in_sem.at[z // 8]
        )
        for z in sorted(range(0, dz, 8), key=lambda z: min(z, dz - 8 - z))
    ]
    for load in loads:
        load.start()
    barrier = pltpu.get_barrier_semaphore()
    neighbours = (dict(a=-1), dict(a=1), dict(b=-1), dict(b=1), dict(c=-1), dict(c=1))
    for offset in neighbours:
        signal(barrier, **offset)
    edge_loads = [
        pltpu.make_async_copy(first_hbm, first, edge_sem.at[0]),
        pltpu.make_async_copy(beyond_hbm, beyond, edge_sem.at[1]),
    ]
    for copy in edge_loads:
        copy.start()

    lane = lax.broadcasted_iota(jnp.int32, (8, dx), 1)
    slot = lane // 8
    left_rim = lane % 8 < 4
    rim_lane = (lane < 4) | (lane >= dx - 4)
    top = jnp.full((8, dx), BINS // 2 - 1.0, jnp.float32)
    core_top = jnp.where(rim_lane, -64.0, top)
    spread = (lax.broadcasted_iota(jnp.int32, (8, dx), 0) * dx + lane) * 389 % 1024
    spread = (spread.astype(jnp.float32) + 0.5) * (1.0 / 1024.0)

    def send(k, src, dst, **offset):
        copy = pltpu.make_async_remote_copy(
            src_ref=src, dst_ref=dst, send_sem=send_sem.at[k], recv_sem=recv_sem.at[k],
            device_id=device(**offset), device_id_type=MESH,
        )
        copy.start()
        return copy

    rows = pl.ds(8, dy)
    planes = pl.ds(4, dz)
    for load in loads[:2]:
        load.wait()
    pl.semaphore_wait(barrier, 6)
    z_rims = [
        send(0, ext.at[pl.ds(4, 4), rows, :], ext.at[pl.ds(4 + dz, 4), rows, :], b=-1),
        send(1, ext.at[pl.ds(dz, 4), rows, :], ext.at[pl.ds(0, 4), rows, :], b=1),
    ]
    for load in loads[2:]:
        load.wait()
    y_rims = [
        send(2, ext.at[planes, pl.ds(8, 4), :], ext.at[planes, pl.ds(8 + dy, 4), :], c=-1),
        send(3, ext.at[planes, pl.ds(4 + dy, 4), :], ext.at[planes, pl.ds(4, 4), :], c=1),
    ]
    for offset in neighbours:
        signal(hop1, **offset)
    acc[...] = jnp.zeros_like(acc)
    for copy in edge_loads:
        copy.wait()
    low_edge = first[0].astype(jnp.float32) * 0.5 - 0.5
    high_edge = beyond[0].astype(jnp.float32) * 0.5 - 0.5

    def classify(square, last, stats):
        wsum, wmax, wmin, wnum = stats
        root = square * (SCALE * SCALE) + 1.0
        magnitude = root * lax.rsqrt(root) - 1.0
        place = jnp.clip(magnitude * (0.5 * BINS / RANGE) - 0.25, 0.0, 0.5 * BINS - 0.5)
        low = jnp.minimum(jnp.floor(place), last)
        share = jnp.floor((place - low) * 512.0 + spread)
        weight = jnp.clip(place - low_edge, 0.0, 0.5) - jnp.clip(place - high_edge, 0.0, 0.5)
        value = weight * magnitude
        stats = (
            wsum + value,
            jnp.maximum(wmax, value),
            jnp.minimum(wmin, magnitude - (2.0 * RANGE) * weight),
            wnum + weight,
        )
        coarse = jnp.floor(low * 0.125)
        fine = low - 8.0 * coarse
        coarse = jnp.concatenate([coarse, coarse - 1.0], axis=0).astype(jnp.bfloat16)
        fine = pair(fine).astype(jnp.bfloat16)
        here = jnp.concatenate(
            [jnp.maximum(256.0 - share, 0.0), jnp.minimum(share, 512.0 - share)], axis=0
        ).astype(jnp.bfloat16)
        after = jnp.concatenate(
            [jnp.maximum(share - 256.0, 0.0), jnp.zeros((8, dx), jnp.float32)], axis=0
        ).astype(jnp.bfloat16)
        one = jnp.ones((16, dx), jnp.bfloat16)
        zero = jnp.zeros((16, dx), jnp.bfloat16)
        coarse_hot = jnp.concatenate(
            [jnp.where(coarse == jnp.bfloat16(2 * k), one, zero) for k in range(8)], axis=0
        )
        hits = [fine == jnp.bfloat16(k) for k in range(8)]
        parts = [jnp.where(hits[0], here, zero)]
        for k in range(1, 8):
            parts.append(jnp.where(hits[k], here, jnp.where(hits[k - 1], after, zero)))
        parts.append(jnp.where(hits[7], after, zero))
        return magnitude, jnp.concatenate(parts, axis=0), coarse_hot, stats

    def count(fines, coarses):
        acc[...] += lax.dot_general(
            jnp.concatenate(coarses, axis=1), jnp.concatenate(fines, axis=1),
            (((1,), (1,)), ((), ())), preferred_element_type=jnp.float32,
        )

    def pack():
        for m in range(dz // 4):
            both = []
            for p in (2 * m, 2 * m + 1):
                out = jnp.zeros((8, dx), jnp.float32)
                for j in range(16):
                    cell = ext[4 + 2 * p + j // 8, pl.ds(8 + 8 * (j % 8), 8), :]
                    out = jnp.where(slot == j, pltpu.roll(cell, 8 * j + 4, 1), out)
                packed[p] = out
                both.append(out)
            to_high[m] = jnp.where(left_rim, both[0], pltpu.roll(both[1], 4, 1))
            to_low[m] = jnp.where(left_rim, pltpu.roll(both[0], dx - 4, 1), both[1])

    def tiles(pairs, stats, fresh):
        fines, coarses = [], []
        for p, which in pairs:
            if fresh:
                out_x = jnp.zeros((8, dx), jnp.float32)
                out_yz = jnp.zeros((8, dx), jnp.float32)
            else:
                out_x, out_yz = rim_x[p], rim_yz[p]
            for j in which:
                z, y = 4 + 2 * p + j // 8, 8 + 8 * (j % 8)
                center = ext[z, pl.ds(y, 8), :]
                for k, coef in enumerate(COEF, start=1):
                    term_x = pltpu.roll(center, dx - k, 1) - pltpu.roll(center, k, 1)
                    term_y = ext[z, pl.ds(y + k, 8), :] - ext[z, pl.ds(y - k, 8), :]
                    term_z = ext[z + k, pl.ds(y, 8), :] - ext[z - k, pl.ds(y, 8), :]
                    grad_x = term_x if k == 1 else grad_x + coef * term_x
                    grad_y = term_y if k == 1 else grad_y + coef * term_y
                    grad_z = term_z if k == 1 else grad_z + coef * term_z
                square_yz = grad_z * grad_z + grad_y * grad_y
                out_x = jnp.where(slot == j, pltpu.roll(grad_x, 8 * j + 4, 1), out_x)
                out_yz = jnp.where(slot == j, pltpu.roll(square_yz, 8 * j + 4, 1), out_yz)
                magnitude, fine_hot, coarse_hot, stats = classify(
                    square_yz + grad_x * grad_x, core_top, stats
                )
                mag_ref[2 * p + j // 8, pl.ds(8 * (j % 8), 8), :] = magnitude
                fines.append(fine_hot)
                coarses.append(coarse_hot)
            rim_x[p] = out_x
            rim_yz[p] = out_yz
        count(fines, coarses)
        return stats

    inner = [j for j in range(16) if 0 < j % 8 < 7]
    outer = [j for j in range(16) if not 0 < j % 8 < 7]
    nothing = jnp.zeros((8, dx), jnp.float32)
    stats = (nothing, nothing, jnp.full((8, dx), 1e30, jnp.float32), nothing)

    def trips(count_of, pairs, which, stats, fresh):
        step = len(pairs) // count_of
        if count_of == 1:
            return tiles([(p, which) for p in pairs], stats, fresh)
        gap = pairs[step] - pairs[0]
        return lax.fori_loop(
            0, count_of, lambda i, s: tiles([(p + gap * i, which) for p in pairs[:step]], s, fresh), stats
        )

    middle = list(range(2, dz // 2 - 2))

    pack()
    x_rims = [
        send(4, to_low, from_high, a=-1),
        send(5, to_high, from_low, a=1),
    ]
    stats = trips(3, middle, inner, stats, True)

    pl.semaphore_wait(hop1, 6)
    if nz > 4:
        signal(near2, b=-2)
        signal(near2, b=2)
        signal(near2, a=2)
    if ny > 4:
        signal(far2, c=-2)
        signal(far2, c=2)

    for copy in y_rims:
        copy.wait_recv()
    stats = trips(1, middle, outer, stats, False)

    turn = (4 - lax.rem(gz, 4)) // 4

    def end_planes(i, stats):
        end = lax.rem(i + turn, 2)
        rim = ext.at[pl.ds((4 + dz) * end, 4), rows, :]
        pltpu.make_async_copy(rim, rim, recv_sem.at[1 - end]).wait()
        at = (dz // 2 - 2) * end
        return tiles([(at, range(16)), (at + 1, range(16))], stats, True)

    stats = lax.fori_loop(0, 2, end_planes, stats)

    if nz > 4:
        pl.semaphore_wait(near2, 3)
        signal(near3, b=4)
    if ny > 4:
        pl.semaphore_wait(far2, 2)
        signal(far3, c=-4)
        signal(far3, c=4)


    rim_stats = (nothing, nothing, jnp.full((8, dx), 1e30, jnp.float32), nothing)

    for copy in x_rims:
        copy.wait_recv()
    fines, coarses = [], []
    for p in range(dz // 2):
        own = packed[p]
        high, low = from_high[p // 2], from_low[p // 2]
        if p % 2:
            low = pltpu.roll(low, dx - 4, 1)
        else:
            high = pltpu.roll(high, 4, 1)
        high = jnp.where(left_rim, 0.0, high - own)
        low = jnp.where(left_rim, low - own, 0.0)
        fix_high = fix_low = None
        for k, coef in enumerate(COEF, start=1):
            more = coef * pltpu.roll(high, dx - k, 1)
            less = coef * pltpu.roll(low, k, 1)
            fix_high = more if fix_high is None else fix_high + more
            fix_low = less if fix_low is None else fix_low + less
        grad_x = rim_x[p] + jnp.where(left_rim, fix_high, -fix_low)
        magnitude, fine_hot, coarse_hot, rim_stats = classify(rim_yz[p] + grad_x * grad_x, top, rim_stats)
        rim_x[p] = magnitude
        fines.append(fine_hot)
        coarses.append(coarse_hot)
    count(fines, coarses)

    wsum = rim_stats[0] + jnp.where(rim_lane, 0.0, stats[0])
    wmax = jnp.maximum(rim_stats[1], jnp.where(rim_lane, 0.0, stats[1]))
    wmin = jnp.minimum(rim_stats[2], jnp.where(rim_lane, 1e30, stats[2]))
    wnum = rim_stats[3] + jnp.where(rim_lane, 0.0, stats[3])

    total = acc[...]
    same = (
        lax.broadcasted_iota(jnp.int32, total.shape, 0) % 8
        == lax.broadcasted_iota(jnp.int32, total.shape, 1) % 8
    )
    total = jnp.where(same, total, 0.0).reshape(16, 8, 144).sum(axis=1)
    source = lax.broadcasted_iota(jnp.int32, (144, 256), 0) // 8
    target = lax.broadcasted_iota(jnp.int32, (144, 256), 1)
    fits = (source == target % 16 + 16 * (target // 128)).astype(jnp.float32).astype(jnp.bfloat16)
    pieces = []
    for _ in range(3):
        pieces.append(total.astype(jnp.bfloat16))
        total = total - pieces[-1].astype(jnp.float32)
    total = lax.dot_general(
        jnp.concatenate(pieces, axis=0), fits, (((1,), (0,)), ((), ())),
        preferred_element_type=jnp.float32,
    )
    total = total[:16] + total[16:32] + total[32:]
    owner = lax.broadcasted_iota(jnp.int32, (16, 128), 1) // 16
    coarse = lax.broadcasted_iota(jnp.int32, (16, 128), 0)

    def bin_row(r):
        mine = jnp.where(coarse == owner + 8 * r, total[:, :128], 0.0)
        carried = jnp.where(coarse + 1 == owner + 8 * r, total[:, 128:], 0.0)
        return (mine + carried).sum(axis=0, keepdims=True) * (1.0 / 256.0)

    row0, row1 = bin_row(0), bin_row(1)
    lane1 = lane[:1]
    row2 = jnp.where(
        lane1 == 0, jnp.min(wmin) + RANGE,
        jnp.where(
            lane1 == 1, jnp.max(wmax) * 2.0,
            jnp.where(lane1 == 2, jnp.sum(wsum), jnp.sum(wnum)) * 2.0,
        ),
    )
    msg[0:3, :] = jnp.concatenate([row0, row1, row2], axis=0)

    def merged(slots, slot_ref):
        value = slot_ref[0]
        added, most, least = value, value, value
        for k in range(1, slots):
            value = slot_ref[k]
            added, most, least = added + value, jnp.maximum(most, value), jnp.minimum(least, value)
        lane3 = lax.broadcasted_iota(jnp.int32, added.shape, 1)
        row3 = lax.broadcasted_iota(jnp.int32, added.shape, 0)
        return jnp.where(
            (row3 < 2) | (lane3 > 1), added, jnp.where(lane3 == 1, most, least)
        )

    def spread_out(peers, slot_ref, send_one, recv_one):
        slot_ref[0] = msg[...]
        for k, offset in enumerate(peers, start=1):
            pltpu.make_async_remote_copy(
                src_ref=msg, dst_ref=slot_ref.at[k], send_sem=send_one, recv_sem=recv_one,
                device_id=device(**offset), device_id_type=MESH,
            ).start()

    def gathered(slots, slot_ref, send_one, recv_one):
        rest = slot_ref.at[pl.ds(1, slots - 1)]
        pltpu.make_async_copy(rest, rest, send_one).wait()
        pltpu.make_async_copy(rest, rest, recv_one).wait()
        return merged(slots, slot_ref)

    def far(a, n):
        return min(a, n - a)

    plane_peers = sorted(
        [(a, b) for a in range(nx) for b in range(nz) if a or b],
        key=lambda ab: -(far(ab[0], nx) + far(ab[1], nz)),
    )
    line_peers = sorted(range(1, ny), key=lambda c: -far(c, ny))

    if nz > 4:
        pl.semaphore_wait(near3, 1)
    spread_out([dict(a=a, b=b) for a, b in plane_peers], plane, plane_send, plane_recv)

    def unpack(i, _):
        for p in (4 * i, 4 * i + 1, 4 * i + 2, 4 * i + 3):
            rim = rim_x[p]
            for j in range(16):
                at = (2 * p + j // 8, pl.ds(8 * (j % 8), 8))
                moved = pltpu.roll(rim, (dx - 8 * j - 4) % dx, 1)
                mag_ref[at] = jnp.where(rim_lane, moved, mag_ref[at])
        return 0

    lax.fori_loop(0, dz // 8, unpack, 0)
    for copy in z_rims + y_rims + x_rims:
        copy.wait_send()

    msg[...] = gathered(nx * nz, plane, plane_send, plane_recv)
    if ny > 4:
        pl.semaphore_wait(far3, 2)
    spread_out([dict(c=c) for c in line_peers], line, line_send, line_recv)
    done = gathered(ny, line, line_send, line_recv)

    hist_ref[pl.ds(0, 128)] = done[0] * (BINS / cells)
    hist_ref[pl.ds(128, 128)] = done[1] * (BINS / cells)
    stat_ref[...] = jnp.where(lane1 < 2, done[2:3], done[2:3] * (1.0 / cells))[0, :4]


def write_out(mag, hist, stat, mag_hbm, hist_hbm, stat_hbm, sems):
    step = mag.shape[0] // 4
    copies = [
        pltpu.make_async_copy(hist, hist_hbm, sems.at[0]),
        pltpu.make_async_copy(stat, stat_hbm, sems.at[1]),
    ]
    for k in range(4):
        part = pl.ds(step * k, step)
        copies.append(pltpu.make_async_copy(mag.at[part], mag_hbm.at[part], sems.at[2 + k]))
    for copy in copies:
        copy.start()
    for copy in copies:
        copy.wait()


def solution(mesh):
    sizes = tuple(mesh.shape[name] for name in ("gx", "gy", "gz"))
    nx, ny, nz = sizes

    def on_device(u, first, beyond):
        dz, dy, dx = u.shape
        cells = u.size * nx * ny * nz
        rims = pltpu.VMEM((dz // 2, 8, dx), jnp.float32)
        half_rims = pltpu.VMEM((dz // 4, 8, dx), jnp.float32)
        mag, hist, stat = pl.pallas_call(
            functools.partial(kernel, sizes, cells),
            out_shape=(
                pltpu.VMEM(u.shape, jnp.float32),
                pltpu.VMEM((BINS,), jnp.float32),
                pltpu.VMEM((4,), jnp.float32),
            ),
            in_specs=[pl.BlockSpec(memory_space=pltpu.HBM)] * 3,
            out_specs=(
                pl.BlockSpec(memory_space=pltpu.VMEM),
                pl.BlockSpec(memory_space=pltpu.VMEM),
                pl.BlockSpec(memory_space=pltpu.VMEM),
            ),
            scratch_shapes=[
                pltpu.VMEM((dz + 8, dy + 16, dx), jnp.float32),
                rims, half_rims, half_rims, half_rims, half_rims, rims, rims,
                pltpu.VMEM((128, 144), jnp.float32),
                pltpu.VMEM((3, 128), jnp.float32),
                pltpu.VMEM((nx * nz, 3, 128), jnp.float32),
                pltpu.VMEM((ny, 3, 128), jnp.float32),
                pltpu.SMEM((1,), jnp.int32),
                pltpu.SMEM((1,), jnp.int32),
                pltpu.SemaphoreType.DMA((dz // 8,)),
                pltpu.SemaphoreType.DMA((2,)),
                pltpu.SemaphoreType.DMA((6,)),
                pltpu.SemaphoreType.DMA((6,)),
                pltpu.SemaphoreType.DMA,
                pltpu.SemaphoreType.DMA,
                pltpu.SemaphoreType.DMA,
                pltpu.SemaphoreType.DMA,
                pltpu.SemaphoreType.REGULAR,
                pltpu.SemaphoreType.REGULAR,
                pltpu.SemaphoreType.REGULAR,
                pltpu.SemaphoreType.REGULAR,
                pltpu.SemaphoreType.REGULAR,
            ],
            compiler_params=pltpu.CompilerParams(collective_id=0, has_side_effects=True),
        )(u, first, beyond)
        mag = pltpu.with_memory_space_constraint(mag, pltpu.VMEM)
        hist = pltpu.with_memory_space_constraint(hist, pltpu.VMEM)
        stat = pltpu.with_memory_space_constraint(stat, pltpu.VMEM)
        return pl.pallas_call(
            write_out,
            out_shape=(
                jax.ShapeDtypeStruct(u.shape, jnp.float32),
                jax.ShapeDtypeStruct((BINS,), jnp.float32),
                jax.ShapeDtypeStruct((4,), jnp.float32),
            ),
            in_specs=[
                pl.BlockSpec(memory_space=pltpu.VMEM),
                pl.BlockSpec(memory_space=pltpu.VMEM),
                pl.BlockSpec(memory_space=pltpu.VMEM),
            ],
            out_specs=[pl.BlockSpec(memory_space=pltpu.HBM)] * 3,
            scratch_shapes=[pltpu.SemaphoreType.DMA((6,))],
        )(mag, hist, stat)

    return jax.shard_map(
        on_device,
        mesh=mesh,
        in_specs=(P("gz", "gy", "gx"), P(), P()),
        out_specs=(P("gz", "gy", "gx"), P(), P()),
        check_vma=False,
    )
```

```python
import functools

import jax
import jax.numpy as jnp
from jax import lax
from jax.experimental import pallas as pl
from jax.experimental.pallas import tpu as pltpu
from jax.sharding import PartitionSpec as P

MESH = pl.DeviceIdType.MESH
BINS = 256
RANGE = 12.0
SCALE = 0.8
COEF = (1.0, -1.0 / 4.0, 1.0 / 21.0, -1.0 / 224.0)


def pair(x):
    return jnp.concatenate([x, x], axis=0)


def kernel(
    sizes, cells, u_hbm, first_hbm, beyond_hbm, mag_ref, hist_ref, stat_ref,
    ext, packed, to_low, to_high, from_low, from_high, rim_x, rim_yz, acc, msg, plane, line, first, beyond,
    in_sem, edge_sem, send_sem, recv_sem, plane_send, plane_recv, line_send, line_recv,
    hop1, near2, near3, far2, far3,
):
    nx, ny, nz = sizes
    dz, dy, dx = u_hbm.shape
    gx, gy, gz = lax.axis_index("gx"), lax.axis_index("gy"), lax.axis_index("gz")

    def device(a=0, c=0, b=0):
        return {
            "gx": lax.rem(gx + (a + nx), nx) if a else gx,
            "gy": lax.rem(gy + (c + ny), ny) if c else gy,
            "gz": lax.rem(gz + (b + nz), nz) if b else gz,
        }

    def signal(sem, **offset):
        pl.semaphore_signal(sem, inc=1, device_id=device(**offset), device_id_type=MESH)

    loads = [
        pltpu.make_async_copy(
            u_hbm.at[pl.ds(z, 8)], ext.at[pl.ds(4 + z, 8), pl.ds(8, dy), :], in_sem.at[z // 8]
        )
        for z in sorted(range(0, dz, 8), key=lambda z: min(z, dz - 8 - z))
    ]
    for load in loads:
        load.start()
    barrier = pltpu.get_barrier_semaphore()
    neighbours = (dict(a=-1), dict(a=1), dict(b=-1), dict(b=1), dict(c=-1), dict(c=1))
    for offset in neighbours:
        signal(barrier, **offset)
    edge_loads = [
        pltpu.make_async_copy(first_hbm, first, edge_sem.at[0]),
        pltpu.make_async_copy(beyond_hbm, beyond, edge_sem.at[1]),
    ]
    for copy in edge_loads:
        copy.start()

    lane = lax.broadcasted_iota(jnp.int32, (8, dx), 1)
    slot = lane // 8
    left_rim = lane % 8 < 4
    rim_lane = (lane < 4) | (lane >= dx - 4)
    top = jnp.full((8, dx), BINS // 2 - 1.0, jnp.float32)
    core_top = jnp.where(rim_lane, -64.0, top)
    spread = (lax.broadcasted_iota(jnp.int32, (8, dx), 0) * dx + lane) * 389 % 1024
    spread = (spread.astype(jnp.float32) + 0.5) * (1.0 / 1024.0)

    def send(k, src, dst, **offset):
        copy = pltpu.make_async_remote_copy(
            src_ref=src, dst_ref=dst, send_sem=send_sem.at[k], recv_sem=recv_sem.at[k],
            device_id=device(**offset), device_id_type=MESH,
        )
        copy.start()
        return copy

    rows = pl.ds(8, dy)
    planes = pl.ds(4, dz)
    for load in loads[:2]:
        load.wait()
    pl.semaphore_wait(barrier, 6)
    z_rims = [
        send(0, ext.at[pl.ds(4, 4), rows, :], ext.at[pl.ds(4 + dz, 4), rows, :], b=-1),
        send(1, ext.at[pl.ds(dz, 4), rows, :], ext.at[pl.ds(0, 4), rows, :], b=1),
    ]
    for load in loads[2:]:
        load.wait()
    y_rims = [
        send(2, ext.at[planes, pl.ds(8, 4), :], ext.at[planes, pl.ds(8 + dy, 4), :], c=-1),
        send(3, ext.at[planes, pl.ds(4 + dy, 4), :], ext.at[planes, pl.ds(4, 4), :], c=1),
    ]
    for offset in neighbours:
        signal(hop1, **offset)
    acc[...] = jnp.zeros_like(acc)
    for copy in edge_loads:
        copy.wait()
    low_edge = first[0].astype(jnp.float32) * 0.5 - 0.5
    high_edge = beyond[0].astype(jnp.float32) * 0.5 - 0.5

    def classify(square, last, stats):
        wsum, wmax, wmin, wnum = stats
        root = square * (SCALE * SCALE) + 1.0
        magnitude = root * lax.rsqrt(root) - 1.0
        place = jnp.clip(magnitude * (0.5 * BINS / RANGE) - 0.25, 0.0, 0.5 * BINS - 0.5)
        low = jnp.minimum(jnp.floor(place), last)
        share = jnp.floor((place - low) * 512.0 + spread)
        weight = jnp.clip(place - low_edge, 0.0, 0.5) - jnp.clip(place - high_edge, 0.0, 0.5)
        value = weight * magnitude
        stats = (
            wsum + value,
            jnp.maximum(wmax, value),
            jnp.minimum(wmin, magnitude - (2.0 * RANGE) * weight),
            wnum + weight,
        )
        coarse = jnp.floor(low * 0.125)
        fine = low - 8.0 * coarse
        coarse = jnp.concatenate([coarse, coarse - 1.0], axis=0).astype(jnp.bfloat16)
        fine = pair(fine).astype(jnp.bfloat16)
        here = jnp.concatenate(
            [jnp.maximum(256.0 - share, 0.0), jnp.minimum(share, 512.0 - share)], axis=0
        ).astype(jnp.bfloat16)
        after = jnp.concatenate(
            [jnp.maximum(share - 256.0, 0.0), jnp.zeros((8, dx), jnp.float32)], axis=0
        ).astype(jnp.bfloat16)
        one = jnp.ones((16, dx), jnp.bfloat16)
        zero = jnp.zeros((16, dx), jnp.bfloat16)
        coarse_hot = jnp.concatenate(
            [jnp.where(coarse == jnp.bfloat16(2 * k), one, zero) for k in range(8)], axis=0
        )
        hits = [fine == jnp.bfloat16(k) for k in range(8)]
        parts = [jnp.where(hits[0], here, zero)]
        for k in range(1, 8):
            parts.append(jnp.where(hits[k], here, jnp.where(hits[k - 1], after, zero)))
        parts.append(jnp.where(hits[7], after, zero))
        return magnitude, jnp.concatenate(parts, axis=0), coarse_hot, stats

    def count(fines, coarses):
        acc[...] += lax.dot_general(
            jnp.concatenate(coarses, axis=1), jnp.concatenate(fines, axis=1),
            (((1,), (1,)), ((), ())), preferred_element_type=jnp.float32,
        )

    def pack():
        for m in range(dz // 4):
            both = []
            for p in (2 * m, 2 * m + 1):
                out = jnp.zeros((8, dx), jnp.float32)
                for j in range(16):
                    cell = ext[4 + 2 * p + j // 8, pl.ds(8 + 8 * (j % 8), 8), :]
                    out = jnp.where(slot == j, pltpu.roll(cell, 8 * j + 4, 1), out)
                packed[p] = out
                both.append(out)
            to_high[m] = jnp.where(left_rim, both[0], pltpu.roll(both[1], 4, 1))
            to_low[m] = jnp.where(left_rim, pltpu.roll(both[0], dx - 4, 1), both[1])

    def tiles(pairs, stats, fresh):
        fines, coarses = [], []
        for p, which in pairs:
            if fresh:
                out_x = jnp.zeros((8, dx), jnp.float32)
                out_yz = jnp.zeros((8, dx), jnp.float32)
            else:
                out_x, out_yz = rim_x[p], rim_yz[p]
            for j in which:
                z, y = 4 + 2 * p + j // 8, 8 + 8 * (j % 8)
                center = ext[z, pl.ds(y, 8), :]
                for k, coef in enumerate(COEF, start=1):
                    term_x = pltpu.roll(center, dx - k, 1) - pltpu.roll(center, k, 1)
                    term_y = ext[z, pl.ds(y + k, 8), :] - ext[z, pl.ds(y - k, 8), :]
                    term_z = ext[z + k, pl.ds(y, 8), :] - ext[z - k, pl.ds(y, 8), :]
                    grad_x = term_x if k == 1 else grad_x + coef * term_x
                    grad_y = term_y if k == 1 else grad_y + coef * term_y
                    grad_z = term_z if k == 1 else grad_z + coef * term_z
                square_yz = grad_z * grad_z + grad_y * grad_y
                out_x = jnp.where(slot == j, pltpu.roll(grad_x, 8 * j + 4, 1), out_x)
                out_yz = jnp.where(slot == j, pltpu.roll(square_yz, 8 * j + 4, 1), out_yz)
                magnitude, fine_hot, coarse_hot, stats = classify(
                    square_yz + grad_x * grad_x, core_top, stats
                )
                mag_ref[2 * p + j // 8, pl.ds(8 * (j % 8), 8), :] = magnitude
                fines.append(fine_hot)
                coarses.append(coarse_hot)
            rim_x[p] = out_x
            rim_yz[p] = out_yz
        count(fines, coarses)
        return stats

    inner = [j for j in range(16) if 0 < j % 8 < 7]
    outer = [j for j in range(16) if not 0 < j % 8 < 7]
    nothing = jnp.zeros((8, dx), jnp.float32)
    stats = (nothing, nothing, jnp.full((8, dx), 1e30, jnp.float32), nothing)

    def trips(count_of, pairs, which, stats, fresh):
        step = len(pairs) // count_of
        if count_of == 1:
            return tiles([(p, which) for p in pairs], stats, fresh)
        gap = pairs[step] - pairs[0]
        return lax.fori_loop(
            0, count_of, lambda i, s: tiles([(p + gap * i, which) for p in pairs[:step]], s, fresh), stats
        )

    middle = list(range(2, dz // 2 - 2))

    pack()
    x_rims = [
        send(4, to_low, from_high, a=-1),
        send(5, to_high, from_low, a=1),
    ]
    stats = trips(3, middle, inner, stats, True)

    pl.semaphore_wait(hop1, 6)
    if nz > 4:
        signal(near2, b=-2)
        signal(near2, b=2)
        signal(near2, a=2)
    if ny > 4:
        signal(far2, c=-2)
        signal(far2, c=2)

    for copy in y_rims:
        copy.wait_recv()
    stats = trips(1, middle, outer, stats, False)

    turn = (4 - lax.rem(gz, 4)) // 4

    def end_planes(i, stats):
        end = lax.rem(i + turn, 2)
        rim = ext.at[pl.ds((4 + dz) * end, 4), rows, :]
        pltpu.make_async_copy(rim, rim, recv_sem.at[1 - end]).wait()
        at = (dz // 2 - 2) * end
        return tiles([(at, range(16)), (at + 1, range(16))], stats, True)

    stats = lax.fori_loop(0, 2, end_planes, stats)

    if nz > 4:
        pl.semaphore_wait(near2, 3)
        signal(near3, b=4)
    if ny > 4:
        pl.semaphore_wait(far2, 2)
        signal(far3, c=-4)
        signal(far3, c=4)


    rim_stats = (nothing, nothing, jnp.full((8, dx), 1e30, jnp.float32), nothing)

    for copy in x_rims:
        copy.wait_recv()
    fines, coarses = [], []
    for p in range(dz // 2):
        own = packed[p]
        high, low = from_high[p // 2], from_low[p // 2]
        if p % 2:
            low = pltpu.roll(low, dx - 4, 1)
        else:
            high = pltpu.roll(high, 4, 1)
        high = jnp.where(left_rim, 0.0, high - own)
        low = jnp.where(left_rim, low - own, 0.0)
        fix_high = fix_low = None
        for k, coef in enumerate(COEF, start=1):
            more = coef * pltpu.roll(high, dx - k, 1)
            less = coef * pltpu.roll(low, k, 1)
            fix_high = more if fix_high is None else fix_high + more
            fix_low = less if fix_low is None else fix_low + less
        grad_x = rim_x[p] + jnp.where(left_rim, fix_high, -fix_low)
        magnitude, fine_hot, coarse_hot, rim_stats = classify(rim_yz[p] + grad_x * grad_x, top, rim_stats)
        rim_x[p] = magnitude
        fines.append(fine_hot)
        coarses.append(coarse_hot)
    count(fines, coarses)

    wsum = rim_stats[0] + jnp.where(rim_lane, 0.0, stats[0])
    wmax = jnp.maximum(rim_stats[1], jnp.where(rim_lane, 0.0, stats[1]))
    wmin = jnp.minimum(rim_stats[2], jnp.where(rim_lane, 1e30, stats[2]))
    wnum = rim_stats[3] + jnp.where(rim_lane, 0.0, stats[3])

    total = acc[...]
    same = (
        lax.broadcasted_iota(jnp.int32, total.shape, 0) % 8
        == lax.broadcasted_iota(jnp.int32, total.shape, 1) % 8
    )
    total = jnp.where(same, total, 0.0).reshape(16, 8, 144).sum(axis=1)
    source = lax.broadcasted_iota(jnp.int32, (144, 256), 0) // 8
    target = lax.broadcasted_iota(jnp.int32, (144, 256), 1)
    fits = (source == target % 16 + 16 * (target // 128)).astype(jnp.float32).astype(jnp.bfloat16)
    pieces = []
    for _ in range(3):
        pieces.append(total.astype(jnp.bfloat16))
        total = total - pieces[-1].astype(jnp.float32)
    total = lax.dot_general(
        jnp.concatenate(pieces, axis=0), fits, (((1,), (0,)), ((), ())),
        preferred_element_type=jnp.float32,
    )
    total = total[:16] + total[16:32] + total[32:]
    owner = lax.broadcasted_iota(jnp.int32, (16, 128), 1) // 16
    coarse = lax.broadcasted_iota(jnp.int32, (16, 128), 0)

    def bin_row(r):
        mine = jnp.where(coarse == owner + 8 * r, total[:, :128], 0.0)
        carried = jnp.where(coarse + 1 == owner + 8 * r, total[:, 128:], 0.0)
        return (mine + carried).sum(axis=0, keepdims=True) * (1.0 / 256.0)

    row0, row1 = bin_row(0), bin_row(1)
    lane1 = lane[:1]
    row2 = jnp.where(
        lane1 == 0, jnp.min(wmin) + RANGE,
        jnp.where(
            lane1 == 1, jnp.max(wmax) * 2.0,
            jnp.where(lane1 == 2, jnp.sum(wsum), jnp.sum(wnum)) * 2.0,
        ),
    )
    msg[0:3, :] = jnp.concatenate([row0, row1, row2], axis=0)

    def merged(slots, slot_ref):
        values = [slot_ref[k] for k in range(slots)]

        def tree(combine):
            level = values
            while len(level) > 1:
                level = [combine(x, y) for x, y in zip(level[::2], level[1::2])] + (
                    level[-1:] if len(level) % 2 else []
                )
            return level[0]

        added, most, least = tree(jnp.add), tree(jnp.maximum), tree(jnp.minimum)
        lane3 = lax.broadcasted_iota(jnp.int32, added.shape, 1)
        row3 = lax.broadcasted_iota(jnp.int32, added.shape, 0)
        return jnp.where(
            (row3 < 2) | (lane3 > 1), added, jnp.where(lane3 == 1, most, least)
        )

    def spread_out(peers, slot_ref, send_one, recv_one):
        for k, offset in enumerate(peers, start=1):
            pltpu.make_async_remote_copy(
                src_ref=msg, dst_ref=slot_ref.at[k], send_sem=send_one, recv_sem=recv_one,
                device_id=device(**offset), device_id_type=MESH,
            ).start()
        slot_ref[0] = msg[...]

    def gathered(slots, slot_ref, send_one, recv_one):
        rest = slot_ref.at[pl.ds(1, slots - 1)]
        pltpu.make_async_copy(rest, rest, send_one).wait()
        pltpu.make_async_copy(rest, rest, recv_one).wait()
        return merged(slots, slot_ref)

    def far(a, n):
        return min(a, n - a)

    plane_peers = sorted(
        [(a, b) for a in range(nx) for b in range(nz) if a or b],
        key=lambda ab: -(far(ab[0], nx) + far(ab[1], nz)),
    )
    line_peers = sorted(range(1, ny), key=lambda c: -far(c, ny))

    if nz > 4:
        pl.semaphore_wait(near3, 1)
    spread_out([dict(a=a, b=b) for a, b in plane_peers], plane, plane_send, plane_recv)

    def unpack(i, _):
        for p in (4 * i, 4 * i + 1, 4 * i + 2, 4 * i + 3):
            rim = rim_x[p]
            for j in range(16):
                at = (2 * p + j // 8, pl.ds(8 * (j % 8), 8))
                moved = pltpu.roll(rim, (dx - 8 * j - 4) % dx, 1)
                mag_ref[at] = jnp.where(rim_lane, moved, mag_ref[at])
        return 0

    lax.fori_loop(0, dz // 8, unpack, 0)
    for copy in z_rims + y_rims + x_rims:
        copy.wait_send()

    msg[...] = gathered(nx * nz, plane, plane_send, plane_recv)
    if ny > 4:
        pl.semaphore_wait(far3, 2)
    spread_out([dict(c=c) for c in line_peers], line, line_send, line_recv)
    done = gathered(ny, line, line_send, line_recv)

    hist_ref[pl.ds(0, 128)] = done[0] * (BINS / cells)
    hist_ref[pl.ds(128, 128)] = done[1] * (BINS / cells)
    stat_ref[...] = jnp.where(lane1 < 2, done[2:3], done[2:3] * (1.0 / cells))[0, :4]


def write_out(mag, hist, stat, mag_hbm, hist_hbm, stat_hbm, sems):
    step = mag.shape[0] // 4
    copies = [
        pltpu.make_async_copy(hist, hist_hbm, sems.at[0]),
        pltpu.make_async_copy(stat, stat_hbm, sems.at[1]),
    ]
    for k in range(4):
        part = pl.ds(step * k, step)
        copies.append(pltpu.make_async_copy(mag.at[part], mag_hbm.at[part], sems.at[2 + k]))
    for copy in copies:
        copy.start()
    for copy in copies:
        copy.wait()


def solution(mesh):
    sizes = tuple(mesh.shape[name] for name in ("gx", "gy", "gz"))
    nx, ny, nz = sizes

    def on_device(u, first, beyond):
        dz, dy, dx = u.shape
        cells = u.size * nx * ny * nz
        rims = pltpu.VMEM((dz // 2, 8, dx), jnp.float32)
        half_rims = pltpu.VMEM((dz // 4, 8, dx), jnp.float32)
        mag, hist, stat = pl.pallas_call(
            functools.partial(kernel, sizes, cells),
            out_shape=(
                pltpu.VMEM(u.shape, jnp.float32),
                pltpu.VMEM((BINS,), jnp.float32),
                pltpu.VMEM((4,), jnp.float32),
            ),
            in_specs=[pl.BlockSpec(memory_space=pltpu.HBM)] * 3,
            out_specs=(
                pl.BlockSpec(memory_space=pltpu.VMEM),
                pl.BlockSpec(memory_space=pltpu.VMEM),
                pl.BlockSpec(memory_space=pltpu.VMEM),
            ),
            scratch_shapes=[
                pltpu.VMEM((dz + 8, dy + 16, dx), jnp.float32),
                rims, half_rims, half_rims, half_rims, half_rims, rims, rims,
                pltpu.VMEM((128, 144), jnp.float32),
                pltpu.VMEM((3, 128), jnp.float32),
                pltpu.VMEM((nx * nz, 3, 128), jnp.float32),
                pltpu.VMEM((ny, 3, 128), jnp.float32),
                pltpu.SMEM((1,), jnp.int32),
                pltpu.SMEM((1,), jnp.int32),
                pltpu.SemaphoreType.DMA((dz // 8,)),
                pltpu.SemaphoreType.DMA((2,)),
                pltpu.SemaphoreType.DMA((6,)),
                pltpu.SemaphoreType.DMA((6,)),
                pltpu.SemaphoreType.DMA,
                pltpu.SemaphoreType.DMA,
                pltpu.SemaphoreType.DMA,
                pltpu.SemaphoreType.DMA,
                pltpu.SemaphoreType.REGULAR,
                pltpu.SemaphoreType.REGULAR,
                pltpu.SemaphoreType.REGULAR,
                pltpu.SemaphoreType.REGULAR,
                pltpu.SemaphoreType.REGULAR,
            ],
            compiler_params=pltpu.CompilerParams(collective_id=0, has_side_effects=True),
        )(u, first, beyond)
        mag = pltpu.with_memory_space_constraint(mag, pltpu.VMEM)
        hist = pltpu.with_memory_space_constraint(hist, pltpu.VMEM)
        stat = pltpu.with_memory_space_constraint(stat, pltpu.VMEM)
        return pl.pallas_call(
            write_out,
            out_shape=(
                jax.ShapeDtypeStruct(u.shape, jnp.float32),
                jax.ShapeDtypeStruct((BINS,), jnp.float32),
                jax.ShapeDtypeStruct((4,), jnp.float32),
            ),
            in_specs=[
                pl.BlockSpec(memory_space=pltpu.VMEM),
                pl.BlockSpec(memory_space=pltpu.VMEM),
                pl.BlockSpec(memory_space=pltpu.VMEM),
            ],
            out_specs=[pl.BlockSpec(memory_space=pltpu.HBM)] * 3,
            scratch_shapes=[pltpu.SemaphoreType.DMA((6,))],
        )(mag, hist, stat)

    return jax.shard_map(
        on_device,
        mesh=mesh,
        in_specs=(P("gz", "gy", "gx"), P(), P()),
        out_specs=(P("gz", "gy", "gx"), P(), P()),
        check_vma=False,
    )
```
